128 devices in a mesh: dp: 16 (over x, y_hi, core), mp: 8 (over y_lo, z).
Axes of the slice: x: 4, y: 4 (y_hi: 2, y_lo: 2; y = y_hi * 2 + y_lo), z: 4, core: 2. Of those that a mesh axis runs over, the one named last changes fastest.
Arguments:
- tokens: bfloat16 [12288, 6144], P('dp', 'mp'), may hold values from -6 to 6
- ln_gain: bfloat16 [6144], P('mp'), may hold values from 0.5 to 1.5
- weights: bfloat16 [6144, 12288], P('dp', 'mp'), may hold values from -0.078125 to 0.078125
- grad_partials: bfloat16 [16, 6144, 12288], P('dp', None, 'mp'), may hold values from -40 to 40, as said below
Outputs:
- hidden: bfloat16 [12288, 12288], P('dp', 'mp')
- perturbed_weights: bfloat16 [6144, 12288], P('dp', 'mp')
The draws below stay inside these ranges and needn't reach their ends.
Inputs may be any that keep to these rules, and one draw needn't show every extreme that they name: `grad_partials`: each slice along the first dimension is one data shard's gradient.
All inputs are finite; a program needn't handle non-finite values.
Results may differ from the reference program's by a relative error of at most 0.012.
Values may be sent and summed in bfloat16 or wider, within the bound.
A program may use at most 192 MiB of HBM per device.

```python
import math
import jax
import jax.numpy as jnp
from jax import lax

D = 6144
FF = 12288
TOKENS = 12288
N_DP = 16
N_MP = 8


def draw_grad_partials(key, part):
    key_rows, key_cols, key_own = jax.random.split(key, 3)
    row_scale = jnp.exp(jax.random.uniform(key_rows, (1, D, 1), jnp.float32, 0.0, math.log(10.0)))
    col_scale = jnp.exp(jax.random.uniform(key_cols, (1, 1, FF), jnp.float32, 0.0, math.log(10.0)))
    ramp = (3.0 ** (jnp.arange(N_DP, dtype=jnp.float32) / max(N_DP - 1, 1))).reshape(N_DP, 1, 1)
    row_place = (jnp.arange(D, dtype=jnp.float32) / D).reshape(1, D, 1)
    block_width = FF // N_MP
    col_place = ((jnp.arange(FF) % block_width).astype(jnp.float32) / block_width).reshape(1, 1, FF)
    rise = 3.0
    own = jnp.clip(jax.random.normal(key_own, (N_DP, D, FF), jnp.float32), -6.0, 6.0)
    values = ramp * row_scale * col_scale * own
    position = rise ** (row_place - 1.0) * rise ** (col_place - 1.0)
    return (0.01 * values * position).astype(jnp.bfloat16)


def block_scale(stream_key, dims, cuts, smallest, largest):
    gain, own = 1.0, jax.random.fold_in(stream_key, 6)
    for axis_at, parts in cuts:
        draws = jnp.exp(jax.random.uniform(jax.random.fold_in(own, axis_at), (parts,), jnp.float32, smallest / len(cuts), largest / len(cuts)))
        gain = gain * jnp.repeat(draws, dims[axis_at] // parts).reshape([-1 if axis == axis_at else 1 for axis in range(len(dims))])
    return gain


def noise(stream_key, extent, scale, limit, shards=(), held_as=jnp.bfloat16):
    factor_of = block_scale(stream_key, extent, shards, -0.22, 0.18) if shards else 1.0
    drawn = jax.random.normal(stream_key, extent, jnp.float32) * scale * factor_of
    return jnp.minimum(jnp.maximum(drawn, -limit), limit).astype(held_as)


def setup_inputs(seed: int = 0) -> dict:
    arg_keys = jax.random.split(jax.random.key(seed), 5)
    return {
        "tokens": noise(arg_keys[0], (TOKENS, D), 1.0, 6.0, ((0, 16), (1, 8))),
        "ln_gain": jnp.clip(1.0 + 0.1 * jax.random.normal(arg_keys[1], (D,), jnp.float32), 0.5, 1.5).astype(jnp.bfloat16),
        "weights": noise(arg_keys[2], (D, FF), D ** -0.5, 0.078125, ((0, 16), (1, 8))),
        "grad_partials": draw_grad_partials(jax.random.fold_in(arg_keys[4], 71), 0),
    }


def reference(tokens, ln_gain, weights, grad_partials):

    def add_shard(index, total):
        return total + grad_partials[index].astype(jnp.float32)
    grad = lax.fori_loop(0, N_DP, add_shard, jnp.zeros((D, FF), jnp.float32))
    squares = jnp.sum(grad * grad)
    scale = 0.7 * math.sqrt(FF) / jnp.sqrt(squares + 1e-12)
    perturbed = (weights.astype(jnp.float32) + scale * grad).astype(jnp.bfloat16)
    values = tokens.astype(jnp.float32)
    center = lax.optimization_barrier(jnp.mean(values, axis=1, keepdims=True))
    spread = lax.optimization_barrier(jnp.mean((values - center) ** 2, axis=1, keepdims=True))
    normed = ((values - center) / jnp.sqrt(spread + 1e-06) * ln_gain.astype(jnp.float32)).astype(jnp.bfloat16)
    pre = jnp.dot(normed, perturbed, preferred_element_type=jnp.float32)
    hidden = jax.nn.gelu(pre, approximate=False).astype(jnp.bfloat16)
    return (hidden, perturbed)
```

```python
import functools
import math

import jax
import jax.numpy as jnp
from jax import lax
from jax.experimental import pallas as pl
from jax.experimental.pallas import tpu as pltpu
from jax.sharding import Mesh
from jax.sharding import PartitionSpec as P

FF = 12288
MP = ("mp_0", "mp_1")
DP = ("dp_0", "dp_1", "dp_2")
AXES = ("dp_0", "dp_1", "dp_2", "mp_0", "mp_1")
MESH = pl.DeviceIdType.MESH

BLK = 384
HALF = BLK // 2
COLS = 1536
TOK = 768
FEAT = 768
NMP = 8
D = FEAT * NMP
CH = 16
F32 = jnp.float32
BF16 = jnp.bfloat16


def kernel(
    tok_hbm, gain_hbm, w_hbm, grad_hbm, hid_hbm, pert_hbm,
    own, oth, xr, yr, tok, gb, gf, wb, pre, hid, nsend, nrecv,
    ssem, rsem, lsem,
):
    x, yh, c, yl, z = [lax.axis_index(a) for a in AXES]
    y = yh * 2 + yl

    def xid(k):
        return {"dp_0": lax.rem(x + k, 4)}

    def yid(k):
        yy = lax.rem(y + k, 4)
        return {"dp_1": yy // 2, "mp_0": lax.rem(yy, 2)}

    def zid(k):
        return {"mp_1": lax.rem(z + k, 4)}

    core = {"dp_2": 1 - c}
    ypair = {"mp_0": 1 - yl}
    yfar = {"dp_1": 1 - yh}

    count = {"s": 0, "l": 0}
    sends = []

    def remote(src, dst, dev):
        i = count["s"]
        count["s"] += 1
        cp = pltpu.make_async_remote_copy(
            src_ref=src, dst_ref=dst, send_sem=ssem.at[i], recv_sem=rsem.at[i],
            device_id=dev, device_id_type=MESH,
        )
        sends.append(cp)
        return cp

    def local(src, dst):
        i = count["l"]
        count["l"] += 1
        cp = pltpu.make_async_copy(src, dst, lsem.at[i])
        cp.start()
        return cp

    def rows(start, n):
        return pl.ds(pl.multiple_of(start, 16), n)

    def block(xk, far):
        yy = 1 - yh if far else yh
        return lax.rem(x + xk, 4) * 2 + yy

    barrier = pltpu.get_barrier_semaphore()
    peers = [core] + [xid(k) for k in (1, 2, 3)] + [yid(k) for k in (1, 2, 3)] + [zid(k) for k in (1, 2, 3)]
    for p in peers:
        pl.semaphore_signal(barrier, inc=1, device_id=p, device_id_type=MESH)
    order = [(2, True), (1, True), (3, True), (2, False), (1, False), (3, False), (0, True), (0, False)]
    mine = []
    for xk, far in order:
        j = block(xk, far)
        mine.append(local(grad_hbm.at[0, rows((2 * j + c) * BLK, BLK), :], own.at[j]))
    me_t = yl * 4 + z
    pa_t = (1 - yl) * 4 + z
    lt = local(tok_hbm, tok.at[me_t])
    lg = local(gain_hbm, gb.at[me_t])
    lw = local(w_hbm, wb)
    pl.semaphore_wait(barrier, len(peers))

    theirs = []
    for xk, far in order:
        j = block(xk, far)
        cp = remote(grad_hbm.at[0, rows((2 * j + 1 - c) * BLK, BLK), :], oth.at[j], core)
        cp.start()
        theirs.append(cp)

    ty = remote(tok_hbm, tok.at[me_t], ypair)
    gy = remote(gain_hbm, gb.at[me_t], ypair)
    ty.start()
    gy.start()
    tz = []
    for k in (1, 3, 2):
        t = remote(tok_hbm, tok.at[me_t], zid(k))
        g = remote(gain_hbm, gb.at[me_t], zid(k))
        t.start()
        g.start()
        tz += [t, g]

    def add_rows(j, r0, extra):
        def body(i, _):
            r = pl.ds(pl.multiple_of(r0 + i * CH, CH), CH)
            v = own[j, r, :].astype(F32)
            for ref, base in extra:
                v = v + ref[pl.ds(pl.multiple_of(base + i * CH, CH), CH), :].astype(F32)
            own[j, r, :] = v.astype(BF16)
            return 0

        lax.fori_loop(0, HALF // CH, body, 0)

    def pair_sum(n):
        xk, far = order[n]
        j = block(xk, far)
        mine[n].wait()
        theirs[n].wait_recv()
        return j

    rs = []

    def xsend(j, half, d, slot):
        cp = remote(own.at[j, pl.ds(half * HALF, HALF), :], xr.at[d, slot], xid(1 if d == 0 else 3))
        cp.start()
        rs.append(cp)
        return cp

    fin = {}
    for far in (True, False):
        n0 = 0 if far else 3
        base = 0 if far else 3
        j2 = pair_sum(n0)
        add_rows(j2, 0, [(oth.at[j2], 0)])
        r0 = xsend(j2, 0, 0, base)
        add_rows(j2, HALF, [(oth.at[j2], HALF)])
        l0 = xsend(j2, 1, 1, base)
        jr = pair_sum(n0 + 1)
        add_rows(jr, HALF, [(oth.at[jr], HALF)])
        r1 = xsend(jr, 1, 0, base + 2)
        jl = pair_sum(n0 + 2)
        add_rows(jl, 0, [(oth.at[jl], 0)])
        l1 = xsend(jl, 0, 1, base + 1)
        r0.wait_recv()
        add_rows(jr, 0, [(oth.at[jr], 0), (xr.at[0, base], 0)])
        r2 = xsend(jr, 0, 0, base + 1)
        l0.wait_recv()
        add_rows(jl, HALF, [(oth.at[jl], HALF), (xr.at[1, base], 0)])
        l2 = xsend(jl, 1, 1, base + 2)
        fin[far] = (r1, r2, l1, l2)

    ty.wait_recv()
    gy.wait_recv()
    for k in (1, 3, 2):
        t = remote(tok.at[pa_t], tok.at[pa_t], zid(k))
        g = remote(gb.at[pa_t], gb.at[pa_t], zid(k))
        t.start()
        g.start()
        tz += [t, g]

    jf = pair_sum(6)
    r1, r2, l1, l2 = fin[True]
    r1.wait_recv()
    l1.wait_recv()
    r2.wait_recv()
    ys = []
    for h, last in ((0, None), (1, l2)):
        if last is not None:
            last.wait_recv()
        add_rows(jf, h * HALF, [(oth.at[jf], h * HALF), (xr.at[0, 1 + h], 0), (xr.at[1, 1 + h], 0)])
        cp = remote(own.at[jf, pl.ds(h * HALF, HALF), :], yr.at[h], yfar)
        cp.start()
        ys.append(cp)

    jo = pair_sum(7)
    for cp in fin[False]:
        cp.wait_recv()
    for cp in ys:
        cp.wait_recv()

    def finish(h, acc):
        def body(i, a):
            r = pl.multiple_of(i * CH, CH)
            rh = pl.ds(pl.multiple_of(h * HALF + i * CH, CH), CH)
            v = own[jo, rh, :].astype(F32) + oth[jo, rh, :].astype(F32)
            v = v + xr[0, 4 + h, pl.ds(r, CH), :].astype(F32)
            v = v + xr[1, 4 + h, pl.ds(r, CH), :].astype(F32)
            v = v + yr[h, pl.ds(r, CH), :].astype(F32)
            gf[rh, :] = v
            s = v * v
            s = s[:8] + s[8:]
            t = s[:, :128]
            for k in range(1, COLS // 128):
                t = t + s[:, k * 128:(k + 1) * 128]
            return a + t

        return lax.fori_loop(0, HALF // CH, body, acc)

    acc = finish(0, jnp.zeros((8, 128), F32))
    acc = finish(1, acc)
    for cp in rs + ys + theirs:
        cp.wait_send()

    slot = 0
    for stage, group in enumerate(([core], [xid(k) for k in (1, 2, 3)], [yid(k) for k in (1, 2, 3)], [zid(k) for k in (1, 2, 3)])):
        nsend[stage] = acc
        cps = []
        for p in group:
            cp = remote(nsend.at[stage], nrecv.at[slot], p)
            cp.start()
            cps.append((cp, slot))
            slot += 1
        for cp, s in cps:
            cp.wait_recv()
            acc = acc + nrecv[s]
    squares = jnp.sum(jnp.sum(acc, axis=0, keepdims=True), axis=1, keepdims=True)
    scale = 0.7 * math.sqrt(FF) / jnp.sqrt(squares + 1e-12)

    lw.wait()

    def perturb(h):
        def body(i, _):
            r = pl.ds(pl.multiple_of(h * HALF + i * CH, CH), CH)
            own[jo, r, :] = (wb[r, :].astype(F32) + scale * gf[r, :]).astype(BF16)
            return 0

        lax.fori_loop(0, HALF // CH, body, 0)

    def piece(j, h):
        return own.at[j, pl.ds(h * HALF, HALF), :]

    def hop(j, h, d):
        cp = remote(piece(j, h), piece(j, h), xid(1 if d == 0 else 3))
        cp.start()
        return cp

    d2d = {}

    def across(xk, far, h):
        j = block(xk, far)
        cp = remote(piece(j, h), oth.at[j, pl.ds(h * HALF, HALF), :], core)
        cp.start()
        d2d[xk, far, h] = cp

    jl, jr, j2 = block(3, False), block(1, False), block(2, False)
    jfl, jfr, jf2 = block(3, True), block(1, True), block(2, True)
    perturb(0)
    cr0 = hop(jo, 0, 0)
    yo0 = remote(piece(jo, 0), piece(jo, 0), yfar)
    yo0.start()
    perturb(1)
    cl1 = hop(jo, 1, 1)
    yo1 = remote(piece(jo, 1), piece(jo, 1), yfar)
    yo1.start()
    cr1 = hop(jo, 1, 0)
    cl0 = hop(jo, 0, 1)
    across(0, False, 0)
    across(0, False, 1)
    lp = local(own.at[jo], pert_hbm)

    lt.wait()
    lg.wait()
    for cp in tz:
        cp.wait_recv()

    def norm_rows(i, _):
        r = pl.ds(pl.multiple_of(i * CH, CH), CH)
        tot = tok[0, r, :].astype(F32)
        for k in range(1, NMP):
            tot = tot + tok[k, r, :].astype(F32)
        mean = jnp.sum(tot, axis=1, keepdims=True) * (1.0 / D)
        dev = None
        for k in range(NMP):
            e = tok[k, r, :].astype(F32) - mean
            dev = e * e if dev is None else dev + e * e
        var = jnp.sum(dev, axis=1, keepdims=True) * (1.0 / D)
        inv = 1.0 / jnp.sqrt(var + 1e-6)
        for k in range(NMP):
            e = (tok[k, r, :].astype(F32) - mean) * inv * gb[k, 0:1, :]
            tok[k, r, :] = e.astype(BF16)
        return 0

    for cp in tz:
        cp.wait_send()
    lax.fori_loop(0, TOK // CH, norm_rows, 0)

    cr0.wait_recv()
    fr = hop(jl, 0, 0)
    across(3, False, 0)
    cl1.wait_recv()
    fl = hop(jr, 1, 1)
    across(1, False, 1)
    yo0.wait_recv()
    yo1.wait_recv()
    fr0, fl1 = hop(jf, 0, 0), hop(jf, 1, 1)
    fr1, fl0 = hop(jf, 1, 0), hop(jf, 0, 1)
    across(0, True, 0)
    across(0, True, 1)
    cr1.wait_recv()
    across(3, False, 1)
    cl0.wait_recv()
    across(1, False, 0)

    NT = 256

    def dots(xk, far, n):
        j = block(xk, far)
        cols = pl.ds(pl.multiple_of(n * NT, NT), NT)
        a0 = tok[j, :, pl.ds(pl.multiple_of(c * BLK, BLK), BLK)]
        a1 = tok[j, :, pl.ds(pl.multiple_of((1 - c) * BLK, BLK), BLK)]
        return jnp.dot(a0, own[j, :, cols], preferred_element_type=F32) + jnp.dot(
            a1, oth[j, :, cols], preferred_element_type=F32
        )

    def multiply(xk, far, first=False):
        d2d[xk, far, 0].wait_recv()
        d2d[xk, far, 1].wait_recv()

        def body(n, _):
            cols = pl.ds(pl.multiple_of(n * NT, NT), NT)
            if first:
                pre[:, cols] = dots(xk, far, n)
            else:
                pre[:, cols] = pre[:, cols] + dots(xk, far, n)
            return 0

        lax.fori_loop(0, COLS // NT, body, 0)

    multiply(0, False, True)
    multiply(0, True)
    multiply(3, False)
    multiply(1, False)
    fr.wait_recv()
    across(2, False, 0)
    fl.wait_recv()
    across(2, False, 1)
    fr0.wait_recv()
    ffr = hop(jfl, 0, 0)
    across(3, True, 0)
    fl1.wait_recv()
    ffl = hop(jfr, 1, 1)
    across(1, True, 1)
    multiply(2, False)
    fr1.wait_recv()
    across(3, True, 1)
    fl0.wait_recv()
    across(1, True, 0)
    multiply(3, True)
    multiply(1, True)
    ffr.wait_recv()
    across(2, True, 0)
    ffl.wait_recv()
    across(2, True, 1)
    d2d[2, True, 0].wait_recv()
    d2d[2, True, 1].wait_recv()

    def last(n, _):
        cols = pl.ds(pl.multiple_of(n * NT, NT), NT)
        v = pre[:, cols] + dots(2, True, n)
        hid[:, cols] = (v * 0.5 * (1.0 + lax.erf(v * (1.0 / math.sqrt(2.0))))).astype(BF16)
        return 0

    lax.fori_loop(0, COLS // NT, last, 0)
    lh = local(hid, hid_hbm)
    done = {id(cp) for cp in rs + ys + theirs + tz}
    for cp in sends:
        if id(cp) not in done:
            cp.wait_send()
    lp.wait()
    lh.wait()


NSEM = 84


def per_device(tokens, ln_gain, weights, grad_partials):
    gain = jnp.broadcast_to(ln_gain.astype(F32)[None, :], (8, FEAT))
    anyspace = pl.BlockSpec(memory_space=pl.ANY)
    return pl.pallas_call(
        kernel,
        out_shape=(
            jax.ShapeDtypeStruct((TOK, COLS), BF16),
            jax.ShapeDtypeStruct((BLK, COLS), BF16),
        ),
        in_specs=[anyspace] * 4,
        out_specs=(anyspace, anyspace),
        scratch_shapes=[
            pltpu.VMEM((8, BLK, COLS), BF16),
            pltpu.VMEM((8, BLK, COLS), BF16),
            pltpu.VMEM((2, 6, HALF, COLS), BF16),
            pltpu.VMEM((2, HALF, COLS), BF16),
            pltpu.VMEM((NMP, TOK, FEAT), BF16),
            pltpu.VMEM((NMP, 8, FEAT), F32),
            pltpu.VMEM((BLK, COLS), F32),
            pltpu.VMEM((BLK, COLS), BF16),
            pltpu.VMEM((TOK, COLS), F32),
            pltpu.VMEM((TOK, COLS), BF16),
            pltpu.VMEM((4, 8, 128), F32),
            pltpu.VMEM((10, 8, 128), F32),
            pltpu.SemaphoreType.DMA((NSEM,)),
            pltpu.SemaphoreType.DMA((NSEM,)),
            pltpu.SemaphoreType.DMA((16,)),
        ],
        compiler_params=pltpu.CompilerParams(
            collective_id=0, has_side_effects=True, vmem_limit_bytes=60 * 1024 * 1024
        ),
    )(tokens, gain, weights, grad_partials)


def solution(mesh):
    torus = Mesh(mesh.devices.reshape(4, 2, 2, 2, 4), AXES)
    placed = (P(DP, MP), P(MP), P(DP, MP), P(DP, None, MP))
    return jax.shard_map(
        per_device, mesh=torus, in_specs=placed, out_specs=(P(DP, MP), P(DP, MP)), check_vma=False
    )
```

```python
import functools
import math

import jax
import jax.numpy as jnp
from jax import lax
from jax.experimental import pallas as pl
from jax.experimental.pallas import tpu as pltpu
from jax.sharding import Mesh
from jax.sharding import PartitionSpec as P

FF = 12288
MP = ("mp_0", "mp_1")
DP = ("dp_0", "dp_1", "dp_2")
AXES = ("dp_0", "dp_1", "dp_2", "mp_0", "mp_1")
MESH = pl.DeviceIdType.MESH

BLK = 384
COLS = 1536
TOK = 768
FEAT = 768
NMP = 8
D = FEAT * NMP
SA = 288
SB = BLK - SA
GA = 224
GB = BLK - GA
CH = 16
NT = 256
NSEM = 128
F32 = jnp.float32
BF16 = jnp.bfloat16
R, L = 0, 1


def kernel(
    tok_hbm, gain_hbm, w_hbm, grad_hbm, hid, pert,
    pb, xa, xb, ya, yb, tok, gb, gf, wb, pre, nsend, nrecv,
    ssem, rsem, lsem,
):
    x, yh, c, yl, z = [lax.axis_index(a) for a in AXES]
    y = yh * 2 + yl

    def xid(k):
        return {"dp_0": lax.rem(x + k, 4)}

    def yid(k):
        yy = lax.rem(y + k, 4)
        return {"dp_1": yy // 2, "mp_0": lax.rem(yy, 2)}

    def zid(k):
        return {"mp_1": lax.rem(z + k, 4)}

    core = {"dp_2": 1 - c}
    ypair = {"mp_0": 1 - yl}
    yfar = {"dp_1": 1 - yh}
    xdev = (xid(1), xid(3))

    count = {"s": 0, "l": 0}
    open_sends = []

    def send(src, dst, dev):
        i = count["s"]
        count["s"] += 1
        cp = pltpu.make_async_remote_copy(
            src_ref=src, dst_ref=dst, send_sem=ssem.at[i], recv_sem=rsem.at[i],
            device_id=dev, device_id_type=MESH,
        )
        cp.start()
        open_sends.append(cp)
        return cp

    def local(src, dst):
        i = count["l"]
        count["l"] += 1
        cp = pltpu.make_async_copy(src, dst, lsem.at[i])
        cp.start()
        return cp

    def rows(start, n):
        return pl.ds(pl.multiple_of(start, 16), n)

    mine0 = c * BLK
    peer0 = (1 - c) * BLK
    peer_dst = c * BLK

    def block(xk, far):
        return lax.rem(x + xk, 4) * 2 + ((1 - yh) if far else yh)

    def own(j, r0, n):
        return pb.at[j, rows(mine0 + r0, n), :]

    barrier = pltpu.get_barrier_semaphore()
    chips = [core, *(xid(k) for k in (1, 2, 3)), *({**xid(k), **core} for k in (1, 2, 3))]
    planes = [{**yid(i), **zid(k)} for i in range(4) for k in range(4) if i or k]
    peers = chips + planes
    for p in peers:
        pl.semaphore_signal(barrier, inc=1, device_id=p, device_id_type=MESH)
    order = [(2, True), (1, True), (3, True), (0, True), (2, False), (1, False), (3, False), (0, False)]
    mine = {}
    for key in order:
        j = block(*key)
        mine[key] = local(grad_hbm.at[0, rows(2 * j * BLK + mine0, BLK), :], own(j, 0, BLK))
    me_t, pa_t = yl * 4 + z, (1 - yl) * 4 + z
    lt = local(tok_hbm, tok.at[me_t])
    lg = local(gain_hbm, gb.at[me_t])
    lw = local(w_hbm, wb)
    pl.semaphore_wait(barrier, len(peers))

    theirs = {}
    HA, HB = SA // 2, SB // 2
    for key in order:
        j = block(*key)
        cuts = (0, HA, SA, BLK) if key == order[0] else (0, BLK)
        theirs[key] = [
            send(grad_hbm.at[0, rows(2 * j * BLK + peer0 + lo, hi - lo), :], pb.at[j, rows(peer_dst + lo, hi - lo), :], core)
            for lo, hi in zip(cuts, cuts[1:])
        ]
    ty = send(tok_hbm, tok.at[me_t], ypair)
    t1 = [send(tok_hbm, tok.at[me_t], zid(k)) for k in (1, 3)]
    gy = send(gain_hbm, gb.at[me_t], ypair)
    g1 = [send(gain_hbm, gb.at[me_t], zid(k)) for k in (1, 2, 3)]

    def add(j, r0, n, extra=()):
        def body(i, _):
            r = rows(mine0 + r0 + i * CH, CH)
            v = pb[j, r, :].astype(F32) + pb[j, rows(peer0 + r0 + i * CH, CH), :].astype(F32)
            for ref, base in extra:
                v = v + ref[rows(base + i * CH, CH), :].astype(F32)
            pb[j, r, :] = v.astype(BF16)
            return 0

        lax.fori_loop(0, n // CH, body, 0)

    def ready(key, first=0):
        if not first:
            mine[key].wait()
        theirs[key][first].wait_recv()
        return block(*key)

    def a_send(j, near, half, d, slot):
        return send(own(j, half * HA, HA), xa.at[d, near, slot], xdev[d])

    def b_send(j, half, d, slot):
        return send(own(j, SA + half * HB, HB), xb.at[d, slot], xdev[d])

    rs = []

    def y_send(key):
        j = block(*key)
        xx = lax.rem(x + key[0], 4)
        add(j, SA, SB)
        cp = send(own(j, SA, SB), yb.at[xx], yfar)
        rs.append(cp)
        return cp

    def a_open(far):
        near = 0 if far else 1
        j = ready((2, far))
        add(j, 0, HA)
        r0 = a_send(j, near, 0, R, 0)
        if far:
            ready((2, far), 1)
        add(j, HA, HA)
        l0 = a_send(j, near, 1, L, 0)
        j = ready((1, far))
        add(j, HA, HA)
        r1 = a_send(j, near, 1, R, 2)
        j = ready((3, far))
        add(j, 0, HA)
        l1 = a_send(j, near, 0, L, 1)
        rs.extend((r0, l0, r1, l1))
        return r0, l0, r1, l1

    def a_pass(far, opened):
        near = 0 if far else 1
        r0, l0, r1, l1 = opened
        jr, jl = block(1, far), block(3, far)
        r0.wait_recv()
        add(jr, 0, HA, [(xa.at[R, near, 0], 0)])
        r2 = a_send(jr, near, 0, R, 1)
        l0.wait_recv()
        add(jl, HA, HA, [(xa.at[L, near, 0], 0)])
        l2 = a_send(jl, near, 1, L, 2)
        rs.extend((r2, l2))
        return r1, r2, l1, l2

    far_a = a_open(True)
    yrb = {}
    ready((2, True), 2)
    for xk in (2, 1, 3):
        yrb[xk] = y_send((xk, True))
    ready((0, True))
    yrb[0] = y_send((0, True))
    far_a = a_pass(True, far_a)
    near_a = a_open(False)

    for cp in t1:
        cp.wait_recv()
    TH = TOK // 2
    left_t, right_t = lax.rem(z + 3, 4), lax.rem(z + 1, 4)

    def pass_tokens(base):
        lo = send(tok.at[base + left_t, pl.ds(0, TH), :], tok.at[base + left_t, pl.ds(0, TH), :], zid(1))
        hi = send(tok.at[base + right_t, pl.ds(TH, TH), :], tok.at[base + right_t, pl.ds(TH, TH), :], zid(3))
        return [lo, hi]

    t2 = pass_tokens(yl * 4)

    jf = block(0, True)
    for cp in far_a:
        cp.wait_recv()
    yra = []
    for h in range(2):
        add(jf, h * HA, HA, [(xa.at[R, 0, 1 + h], 0), (xa.at[L, 0, 1 + h], 0)])
        yra.append(send(own(jf, h * HA, HA), ya.at[h], yfar))
    rs += yra

    ty.wait_recv()
    gy.wait_recv()
    t3 = [send(tok.at[pa_t], tok.at[pa_t], zid(k)) for k in (1, 3)]
    g3 = [send(gb.at[pa_t], gb.at[pa_t], zid(k)) for k in (1, 2, 3)]

    near_a = a_pass(False, near_a)

    def b_add(key, half, extra=()):
        j = block(*key)
        xx = lax.rem(x + key[0], 4)
        add(j, SA + half * HB, HB, [(yb.at[xx], half * HB), *extra])
        return j

    yrb[2].wait_recv()
    br0 = b_send(b_add((2, False), 0), 0, R, 0)
    bl0 = b_send(b_add((2, False), 1), 1, L, 0)
    yrb[1].wait_recv()
    br1 = b_send(b_add((1, False), 1), 1, R, 2)
    yrb[3].wait_recv()
    bl1 = b_send(b_add((3, False), 0), 0, L, 1)
    br0.wait_recv()
    br2 = b_send(b_add((1, False), 0, [(xb.at[R, 0], 0)]), 0, R, 1)
    bl0.wait_recv()
    bl2 = b_send(b_add((3, False), 1, [(xb.at[L, 0], 0)]), 1, L, 2)
    rs += [br0, bl0, br1, bl1, br2, bl2]

    jo = ready((0, False))

    def finish(r0, n, extra, acc):
        def body(i, a):
            rh = rows(r0 + i * CH, CH)
            v = pb[jo, rows(mine0 + r0 + i * CH, CH), :].astype(F32) + pb[jo, rows(peer0 + r0 + i * CH, CH), :].astype(F32)
            for ref, base in extra:
                v = v + ref[rows(base + i * CH, CH), :].astype(F32)
            gf[rh, :] = v
            s = v * v
            s = s[:8] + s[8:]
            t = s[:, :128]
            for k in range(1, COLS // 128):
                t = t + s[:, k * 128:(k + 1) * 128]
            return a + t

        return lax.fori_loop(0, n // CH, body, acc)

    acc = jnp.zeros((8, 128), F32)
    for cp in [*near_a, *yra]:
        cp.wait_recv()
    for h in range(2):
        acc = finish(h * HA, HA, [(xa.at[R, 1, 1 + h], 0), (xa.at[L, 1, 1 + h], 0), (ya.at[h], 0)], acc)
    yrb[0].wait_recv()
    for cp in (br1, bl1, br2, bl2):
        cp.wait_recv()
    for h in range(2):
        acc = finish(SA + h * HB, HB, [(yb.at[x], h * HB), (xb.at[R, 1 + h], 0), (xb.at[L, 1 + h], 0)], acc)
    for cp in rs:
        cp.wait_send()
    done = list(rs)

    slot = 0
    for stage, group in enumerate((chips, planes)):
        nsend[stage] = acc
        cps = []
        for p in group:
            cps.append((send(nsend.at[stage], nrecv.at[slot], p), slot))
            slot += 1
        if stage == 1:
            for cp in t3:
                cp.wait_recv()
            t4 = pass_tokens((1 - yl) * 4)
        for cp, s in cps:
            cp.wait_recv()
            acc = acc + nrecv[s]
    squares = jnp.sum(jnp.sum(acc, axis=0, keepdims=True), axis=1, keepdims=True)
    scale = 0.7 * math.sqrt(FF) / jnp.sqrt(squares + 1e-12)

    lw.wait()

    def perturb(i, _):
        r = rows(i * CH, CH)
        v = (wb[r, :].astype(F32) + scale * gf[r, :]).astype(BF16)
        pb[jo, rows(mine0 + i * CH, CH), :] = v
        pert[r, :] = v
        return 0

    PA, PB = GA // 2, GB // 2

    def go(j, r0, n, dev):
        return send(own(j, r0, n), own(j, r0, n), dev)

    d2d = {}

    def across(xk, far, r0, n):
        j = block(xk, far)
        d2d.setdefault((xk, far), []).append(go(j, r0, n, core))

    lax.fori_loop(GA // CH, BLK // CH, perturb, 0)
    ob = [go(jo, GA, GB, xdev[d]) for d in (R, L)]
    lax.fori_loop(0, GA // CH, perturb, 0)
    ya1 = go(jo, 0, GA, yfar)
    oa = [go(jo, 0, GA, xdev[d]) for d in (R, L)]
    across(0, False, 0, BLK)
    yb1 = go(jo, GA, GB, yfar)

    ob[R].wait_recv()
    fb = [go(block(3, False), GA, PB, xdev[R])]
    yl_b = go(block(3, False), GA, GB, yfar)
    across(3, False, GA, GB)
    ob[L].wait_recv()
    fb.append(go(block(1, False), GA + PB, PB, xdev[L]))
    yr_b = go(block(1, False), GA, GB, yfar)
    across(1, False, GA, GB)
    ya1.wait_recv()
    across(0, True, 0, GA)

    lt.wait()
    lg.wait()
    for cp in [*t2, *t4, *g1, *g3]:
        cp.wait_recv()
    tsent = [*t2, *t3, *t4]
    for cp in tsent:
        cp.wait_send()
    done += tsent

    def norm_rows(i, _):
        r = rows(i * CH, CH)
        tot = tok[0, r, :].astype(F32)
        for k in range(1, NMP):
            tot = tot + tok[k, r, :].astype(F32)
        mean = jnp.sum(tot, axis=1, keepdims=True) * (1.0 / D)
        dev = None
        for k in range(NMP):
            e = tok[k, r, :].astype(F32) - mean
            dev = e * e if dev is None else dev + e * e
        var = jnp.sum(dev, axis=1, keepdims=True) * (1.0 / D)
        inv = 1.0 / jnp.sqrt(var + 1e-6)
        for k in range(NMP):
            e = (tok[k, r, :].astype(F32) - mean) * inv * gb[k].astype(F32)
            tok[k, r, :] = e.astype(BF16)
        return 0

    lax.fori_loop(0, TOK // CH, norm_rows, 0)

    def dots(j, n):
        cols = pl.ds(pl.multiple_of(n * NT, NT), NT)
        return jnp.dot(tok[j], pb[j, :, cols], preferred_element_type=F32)

    def multiply(xk, far, first=False):
        j = block(xk, far)
        for cp in d2d[xk, far]:
            cp.wait_recv()

        def body(n, _):
            cols = pl.ds(pl.multiple_of(n * NT, NT), NT)
            if first:
                pre[:, cols] = dots(j, n)
            else:
                pre[:, cols] = pre[:, cols] + dots(j, n)
            return 0

        lax.fori_loop(0, COLS // NT, body, 0)

    oa[R].wait_recv()
    fa = [go(block(3, False), 0, PA, xdev[R])]
    across(3, False, 0, GA)
    oa[L].wait_recv()
    fa.append(go(block(1, False), PA, PA, xdev[L]))
    across(1, False, 0, GA)
    fra = [go(block(0, True), d * PA, PA, xdev[d]) for d in (R, L)]
    frb = [go(block(0, True), (1 - d) * PA, PA, xdev[d]) for d in (R, L)]
    yb1.wait_recv()
    across(0, True, GA, GB)
    fb[R].wait_recv()
    y2 = [go(block(2, False), GA, PB, yfar)]
    across(2, False, GA, PB)
    fb[L].wait_recv()
    y2.append(go(block(2, False), GA + PB, PB, yfar))
    across(2, False, GA + PB, PB)
    multiply(0, False, True)
    multiply(0, True)
    multiply(3, False)
    fa[R].wait_recv()
    across(2, False, 0, PA)
    fa[L].wait_recv()
    across(2, False, PA, PA)
    multiply(1, False)
    yl_b.wait_recv()
    across(3, True, GA, GB)
    yr_b.wait_recv()
    across(1, True, GA, GB)
    fra[R].wait_recv()
    ffa = [go(block(3, True), 0, PA, xdev[R])]
    across(3, True, 0, PA)
    fra[L].wait_recv()
    ffa.append(go(block(1, True), PA, PA, xdev[L]))
    across(1, True, PA, PA)
    multiply(2, False)
    frb[R].wait_recv()
    across(3, True, PA, PA)
    frb[L].wait_recv()
    across(1, True, 0, PA)
    for k in range(2):
        y2[k].wait_recv()
        across(2, True, GA + k * PB, PB)
    multiply(3, True)
    multiply(1, True)
    for k in range(2):
        ffa[k].wait_recv()
        across(2, True, k * PA, PA)
    for cp in d2d[2, True]:
        cp.wait_recv()
    jl = block(2, True)

    def last(n, _):
        cols = pl.ds(pl.multiple_of(n * NT, NT), NT)
        v = pre[:, cols] + dots(jl, n)
        hid[:, cols] = (v * 0.5 * (1.0 + lax.erf(v * (1.0 / math.sqrt(2.0))))).astype(BF16)
        return 0

    lax.fori_loop(0, COLS // NT, last, 0)
    closed = {id(cp) for cp in done}
    for cp in open_sends:
        if id(cp) not in closed:
            cp.wait_send()


def per_device(tokens, ln_gain, weights, grad_partials):
    gain = ln_gain.reshape(1, FEAT)
    hbm = pl.BlockSpec(memory_space=pltpu.HBM)
    return pl.pallas_call(
        kernel,
        out_shape=(
            pltpu.VMEM((TOK, COLS), BF16),
            pltpu.VMEM((BLK, COLS), BF16),
        ),
        in_specs=[hbm] * 4,
        out_specs=(pl.BlockSpec(memory_space=pltpu.VMEM),) * 2,
        scratch_shapes=[
            pltpu.VMEM((8, 2 * BLK, COLS), BF16),
            pltpu.VMEM((2, 2, 3, SA // 2, COLS), BF16),
            pltpu.VMEM((2, 3, SB // 2, COLS), BF16),
            pltpu.VMEM((2, SA // 2, COLS), BF16),
            pltpu.VMEM((4, SB, COLS), BF16),
            pltpu.VMEM((NMP, TOK, FEAT), BF16),
            pltpu.VMEM((NMP, 1, FEAT), BF16),
            pltpu.VMEM((BLK, COLS), F32),
            pltpu.VMEM((BLK, COLS), BF16),
            pltpu.VMEM((TOK, COLS), F32),
            pltpu.VMEM((2, 8, 128), F32),
            pltpu.VMEM((22, 8, 128), F32),
            pltpu.SemaphoreType.DMA((NSEM,)),
            pltpu.SemaphoreType.DMA((NSEM,)),
            pltpu.SemaphoreType.DMA((16,)),
        ],
        compiler_params=pltpu.CompilerParams(
            collective_id=0, has_side_effects=True, vmem_limit_bytes=50 * 1024 * 1024
        ),
    )(tokens, gain, weights, grad_partials)


def solution(mesh):
    torus = Mesh(mesh.devices.reshape(4, 2, 2, 2, 4), AXES)
    placed = (P(DP, MP), P(MP), P(DP, MP), P(DP, None, MP))
    return jax.shard_map(
        per_device, mesh=torus, in_specs=placed, out_specs=(P(DP, MP), P(DP, MP)), check_vma=False
    )
```

```python
import functools
import math

import jax
import jax.numpy as jnp
from jax import lax
from jax.experimental import pallas as pl
from jax.experimental.pallas import tpu as pltpu
from jax.sharding import Mesh
from jax.sharding import PartitionSpec as P

FF = 12288
MP = ("mp_0", "mp_1")
DP = ("dp_0", "dp_1", "dp_2")
AXES = ("dp_0", "dp_1", "dp_2", "mp_0", "mp_1")
MESH = pl.DeviceIdType.MESH

BLK = 384
COLS = 1536
TOK = 768
FEAT = 768
NMP = 8
D = FEAT * NMP
SA = 288
SB = BLK - SA
GA = 224
GB = BLK - GA
CH = 16
NT = 256
NSEM = 128
F32 = jnp.float32
BF16 = jnp.bfloat16
R, L = 0, 1


def kernel(
    tok_hbm, gain_hbm, w_hbm, grad_hbm, hid, pert,
    pb, xa, xb, ya, yb, tok, gb, gf, wb, pre, nsend, nrecv,
    ssem, rsem, lsem,
):
    x, yh, c, yl, z = [lax.axis_index(a) for a in AXES]
    y = yh * 2 + yl

    def xid(k):
        return {"dp_0": lax.rem(x + k, 4)}

    def yid(k):
        yy = lax.rem(y + k, 4)
        return {"dp_1": yy // 2, "mp_0": lax.rem(yy, 2)}

    def zid(k):
        return {"mp_1": lax.rem(z + k, 4)}

    core = {"dp_2": 1 - c}
    ypair = {"mp_0": 1 - yl}
    yfar = {"dp_1": 1 - yh}
    xdev = (xid(1), xid(3))

    count = {"s": 0, "l": 0}
    open_sends = []

    def send(src, dst, dev):
        i = count["s"]
        count["s"] += 1
        cp = pltpu.make_async_remote_copy(
            src_ref=src, dst_ref=dst, send_sem=ssem.at[i], recv_sem=rsem.at[i],
            device_id=dev, device_id_type=MESH,
        )
        cp.start()
        open_sends.append(cp)
        return cp

    def local(src, dst):
        i = count["l"]
        count["l"] += 1
        cp = pltpu.make_async_copy(src, dst, lsem.at[i])
        cp.start()
        return cp

    def rows(start, n):
        return pl.ds(pl.multiple_of(start, 16), n)

    mine0 = c * BLK
    peer0 = (1 - c) * BLK
    peer_dst = c * BLK

    def block(xk, far):
        return lax.rem(x + xk, 4) * 2 + ((1 - yh) if far else yh)

    def own(j, r0, n):
        return pb.at[j, rows(mine0 + r0, n), :]

    barrier = pltpu.get_barrier_semaphore()
    chips = [core, *(xid(k) for k in (1, 2, 3)), *({**xid(k), **core} for k in (1, 2, 3))]
    planes = [{**yid(i), **zid(k)} for i in range(4) for k in range(4) if i or k]
    peers = chips + planes
    for p in peers:
        pl.semaphore_signal(barrier, inc=1, device_id=p, device_id_type=MESH)
    order = [(2, True), (1, True), (3, True), (0, True), (2, False), (1, False), (3, False), (0, False)]
    mine = {}
    for key in order:
        j = block(*key)
        mine[key] = local(grad_hbm.at[0, rows(2 * j * BLK + mine0, BLK), :], own(j, 0, BLK))
    me_t, pa_t = yl * 4 + z, (1 - yl) * 4 + z
    lt = local(tok_hbm, tok.at[me_t])
    lg = local(gain_hbm, gb.at[me_t])
    lw = local(w_hbm, wb)
    pl.semaphore_wait(barrier, len(peers))

    theirs = {}
    HA, HB = SA // 2, SB // 2
    for key in order:
        j = block(*key)
        cuts = (0, HA, SA, BLK) if key == order[0] else (0, BLK)
        theirs[key] = [
            send(grad_hbm.at[0, rows(2 * j * BLK + peer0 + lo, hi - lo), :], pb.at[j, rows(peer_dst + lo, hi - lo), :], core)
            for lo, hi in zip(cuts, cuts[1:])
        ]
    ty = send(tok_hbm, tok.at[me_t], ypair)
    t1 = [send(tok_hbm, tok.at[me_t], zid(k)) for k in (1, 3)]
    gy = send(gain_hbm, gb.at[me_t], ypair)
    g1 = [send(gain_hbm, gb.at[me_t], zid(k)) for k in (1, 2, 3)]

    def add(j, r0, n, extra=()):
        def body(i, _):
            r = rows(mine0 + r0 + i * CH, CH)
            v = pb[j, r, :].astype(F32) + pb[j, rows(peer0 + r0 + i * CH, CH), :].astype(F32)
            for ref, base in extra:
                v = v + ref[rows(base + i * CH, CH), :].astype(F32)
            pb[j, r, :] = v.astype(BF16)
            return 0

        lax.fori_loop(0, n // CH, body, 0)

    def ready(key, first=0):
        if not first:
            mine[key].wait()
        theirs[key][first].wait_recv()
        return block(*key)

    def a_send(j, near, half, d, slot):
        return send(own(j, half * HA, HA), xa.at[d, near, slot], xdev[d])

    def b_send(j, half, d, slot):
        return send(own(j, SA + half * HB, HB), xb.at[d, slot], xdev[d])

    rs = []

    def y_send(key):
        j = block(*key)
        xx = lax.rem(x + key[0], 4)
        add(j, SA, SB)
        cp = send(own(j, SA, SB), yb.at[xx], yfar)
        rs.append(cp)
        return cp

    def a_open(far):
        near = 0 if far else 1
        j = ready((2, far))
        add(j, 0, HA)
        r0 = a_send(j, near, 0, R, 0)
        if far:
            ready((2, far), 1)
        add(j, HA, HA)
        l0 = a_send(j, near, 1, L, 0)
        j = ready((1, far))
        add(j, HA, HA)
        r1 = a_send(j, near, 1, R, 2)
        j = ready((3, far))
        add(j, 0, HA)
        l1 = a_send(j, near, 0, L, 1)
        rs.extend((r0, l0, r1, l1))
        return r0, l0, r1, l1

    def a_pass(far, opened):
        near = 0 if far else 1
        r0, l0, r1, l1 = opened
        jr, jl = block(1, far), block(3, far)
        r0.wait_recv()
        add(jr, 0, HA, [(xa.at[R, near, 0], 0)])
        r2 = a_send(jr, near, 0, R, 1)
        l0.wait_recv()
        add(jl, HA, HA, [(xa.at[L, near, 0], 0)])
        l2 = a_send(jl, near, 1, L, 2)
        rs.extend((r2, l2))
        return r1, r2, l1, l2

    far_a = a_open(True)
    yrb = {}
    ready((2, True), 2)
    for xk in (2, 1, 3):
        yrb[xk] = y_send((xk, True))
    ready((0, True))
    yrb[0] = y_send((0, True))
    far_a = a_pass(True, far_a)
    near_a = a_open(False)

    for cp in t1:
        cp.wait_recv()
    TH = TOK // 2
    left_t, right_t = lax.rem(z + 3, 4), lax.rem(z + 1, 4)

    def pass_tokens(base):
        lo = send(tok.at[base + left_t, pl.ds(0, TH), :], tok.at[base + left_t, pl.ds(0, TH), :], zid(1))
        hi = send(tok.at[base + right_t, pl.ds(TH, TH), :], tok.at[base + right_t, pl.ds(TH, TH), :], zid(3))
        return [lo, hi]

    t2 = pass_tokens(yl * 4)

    jf = block(0, True)
    for cp in far_a:
        cp.wait_recv()
    yra = []
    for h in range(2):
        add(jf, h * HA, HA, [(xa.at[R, 0, 1 + h], 0), (xa.at[L, 0, 1 + h], 0)])
        yra.append(send(own(jf, h * HA, HA), ya.at[h], yfar))
    rs += yra

    ty.wait_recv()
    gy.wait_recv()
    t3 = [send(tok.at[pa_t], tok.at[pa_t], zid(k)) for k in (1, 3)]
    g3 = [send(gb.at[pa_t], gb.at[pa_t], zid(k)) for k in (1, 2, 3)]

    near_a = a_pass(False, near_a)

    def b_add(key, half, extra=()):
        j = block(*key)
        xx = lax.rem(x + key[0], 4)
        add(j, SA + half * HB, HB, [(yb.at[xx], half * HB), *extra])
        return j

    yrb[2].wait_recv()
    br0 = b_send(b_add((2, False), 0), 0, R, 0)
    bl0 = b_send(b_add((2, False), 1), 1, L, 0)
    yrb[1].wait_recv()
    br1 = b_send(b_add((1, False), 1), 1, R, 2)
    yrb[3].wait_recv()
    bl1 = b_send(b_add((3, False), 0), 0, L, 1)
    br0.wait_recv()
    br2 = b_send(b_add((1, False), 0, [(xb.at[R, 0], 0)]), 0, R, 1)
    bl0.wait_recv()
    bl2 = b_send(b_add((3, False), 1, [(xb.at[L, 0], 0)]), 1, L, 2)
    rs += [br0, bl0, br1, bl1, br2, bl2]

    jo = ready((0, False))

    def finish(r0, n, extra, acc):
        def body(i, a):
            rh = rows(r0 + i * CH, CH)
            v = pb[jo, rows(mine0 + r0 + i * CH, CH), :].astype(F32) + pb[jo, rows(peer0 + r0 + i * CH, CH), :].astype(F32)
            for ref, base in extra:
                v = v + ref[rows(base + i * CH, CH), :].astype(F32)
            gf[rh, :] = v
            s = v * v
            s = s[:8] + s[8:]
            t = s[:, :128]
            for k in range(1, COLS // 128):
                t = t + s[:, k * 128:(k + 1) * 128]
            return a + t

        return lax.fori_loop(0, n // CH, body, acc)

    acc = jnp.zeros((8, 128), F32)
    for cp in [*near_a, *yra]:
        cp.wait_recv()
    for h in range(2):
        acc = finish(h * HA, HA, [(xa.at[R, 1, 1 + h], 0), (xa.at[L, 1, 1 + h], 0), (ya.at[h], 0)], acc)
    yrb[0].wait_recv()
    for cp in (br1, bl1, br2, bl2):
        cp.wait_recv()
    for h in range(2):
        acc = finish(SA + h * HB, HB, [(yb.at[x], h * HB), (xb.at[R, 1 + h], 0), (xb.at[L, 1 + h], 0)], acc)
    for cp in rs:
        cp.wait_send()
    done = list(rs)

    slot = 0
    for stage, group in enumerate((chips, planes)):
        nsend[stage] = acc
        cps = []
        for p in group:
            cps.append((send(nsend.at[stage], nrecv.at[slot], p), slot))
            slot += 1
        if stage == 1:
            for cp in t3:
                cp.wait_recv()
            t4 = pass_tokens((1 - yl) * 4)
        for cp, s in cps:
            cp.wait_recv()
            acc = acc + nrecv[s]
    squares = jnp.sum(jnp.sum(acc, axis=0, keepdims=True), axis=1, keepdims=True)
    scale = 0.7 * math.sqrt(FF) / jnp.sqrt(squares + 1e-12)

    lw.wait()

    def perturb(i, _):
        r = rows(i * CH, CH)
        v = (wb[r, :].astype(F32) + scale * gf[r, :]).astype(BF16)
        pb[jo, rows(mine0 + i * CH, CH), :] = v
        pert[r, :] = v
        return 0

    PA, PB = GA // 2, GB // 2

    def go(j, r0, n, dev, c0=0, cn=COLS):
        ref = pb.at[j, rows(mine0 + r0, n), pl.ds(c0, cn)]
        return send(ref, ref, dev)

    d2d = {}

    def across(xk, far, r0, n, part=0, c0=0, cn=COLS):
        j = block(xk, far)
        d2d.setdefault((xk, far, part), []).append(go(j, r0, n, core, c0, cn))

    lax.fori_loop(GA // CH, BLK // CH, perturb, 0)
    ob = [go(jo, GA, GB, xdev[d]) for d in (R, L)]
    lax.fori_loop(0, GA // CH, perturb, 0)
    ya1 = go(jo, 0, GA, yfar)
    oa = [go(jo, 0, GA, xdev[d]) for d in (R, L)]
    across(0, False, 0, BLK)
    yb1 = go(jo, GA, GB, yfar)

    ob[R].wait_recv()
    fb = [go(block(3, False), GA, PB, xdev[R])]
    yl_b = go(block(3, False), GA, GB, yfar)
    across(3, False, GA, GB)
    ob[L].wait_recv()
    fb.append(go(block(1, False), GA + PB, PB, xdev[L]))
    yr_b = go(block(1, False), GA, GB, yfar)
    across(1, False, GA, GB)
    ya1.wait_recv()
    across(0, True, 0, GA)

    lt.wait()
    lg.wait()
    for cp in [*t2, *t4, *g1, *g3]:
        cp.wait_recv()
    tsent = [*t2, *t3, *t4]
    for cp in tsent:
        cp.wait_send()
    done += tsent

    def norm_rows(i, _):
        r = rows(i * CH, CH)
        tot = tok[0, r, :].astype(F32)
        for k in range(1, NMP):
            tot = tot + tok[k, r, :].astype(F32)
        mean = jnp.sum(tot, axis=1, keepdims=True) * (1.0 / D)
        dev = None
        for k in range(NMP):
            e = tok[k, r, :].astype(F32) - mean
            dev = e * e if dev is None else dev + e * e
        var = jnp.sum(dev, axis=1, keepdims=True) * (1.0 / D)
        inv = 1.0 / jnp.sqrt(var + 1e-6)
        for k in range(NMP):
            e = (tok[k, r, :].astype(F32) - mean) * inv * gb[k].astype(F32)
            tok[k, r, :] = e.astype(BF16)
        return 0

    lax.fori_loop(0, TOK // CH, norm_rows, 0)

    def dots(j, n):
        cols = pl.ds(pl.multiple_of(n * NT, NT), NT)
        return jnp.dot(tok[j], pb[j, :, cols], preferred_element_type=F32)

    def multiply(xk, far, first=False):
        j = block(xk, far)
        for cp in d2d[xk, far, 0]:
            cp.wait_recv()

        def body(n, _):
            cols = pl.ds(pl.multiple_of(n * NT, NT), NT)
            if first:
                pre[:, cols] = dots(j, n)
            else:
                pre[:, cols] = pre[:, cols] + dots(j, n)
            return 0

        lax.fori_loop(0, COLS // NT, body, 0)

    oa[R].wait_recv()
    fa = [go(block(3, False), 0, PA, xdev[R])]
    across(3, False, 0, GA)
    oa[L].wait_recv()
    fa.append(go(block(1, False), PA, PA, xdev[L]))
    across(1, False, 0, GA)
    fra = [go(block(0, True), d * PA, PA, xdev[d]) for d in (R, L)]
    frb = [go(block(0, True), (1 - d) * PA, PA, xdev[d]) for d in (R, L)]
    yb1.wait_recv()
    across(0, True, GA, GB)
    fb[R].wait_recv()
    y2 = [go(block(2, False), GA, PB, yfar)]
    across(2, False, GA, PB)
    fb[L].wait_recv()
    y2.append(go(block(2, False), GA + PB, PB, yfar))
    across(2, False, GA + PB, PB)
    multiply(0, False, True)
    multiply(0, True)
    multiply(3, False)
    fa[R].wait_recv()
    across(2, False, 0, PA)
    fa[L].wait_recv()
    across(2, False, PA, PA)
    multiply(1, False)
    yl_b.wait_recv()
    across(3, True, GA, GB)
    yr_b.wait_recv()
    across(1, True, GA, GB)
    CN = COLS // 2
    fra[R].wait_recv()
    ffa = [[go(block(3, True), 0, PA, xdev[R], q * CN, CN) for q in range(2)]]
    across(3, True, 0, PA)
    fra[L].wait_recv()
    ffa.append([go(block(1, True), PA, PA, xdev[L], q * CN, CN) for q in range(2)])
    across(1, True, PA, PA)
    multiply(2, False)
    frb[R].wait_recv()
    across(3, True, PA, PA)
    frb[L].wait_recv()
    across(1, True, 0, PA)
    multiply(3, True)
    for k in range(2):
        y2[k].wait_recv()
        across(2, True, GA + k * PB, PB)
    for k in range(2):
        ffa[k][0].wait_recv()
        across(2, True, k * PA, PA, 0, 0, CN)
    multiply(1, True)
    for k in range(2):
        ffa[k][1].wait_recv()
        across(2, True, k * PA, PA, 1, CN, CN)
    jl = block(2, True)

    def last(n, _):
        cols = pl.ds(pl.multiple_of(n * NT, NT), NT)
        v = pre[:, cols] + dots(jl, n)
        hid[:, cols] = (v * 0.5 * (1.0 + lax.erf(v * (1.0 / math.sqrt(2.0))))).astype(BF16)
        return 0

    for q in range(2):
        for cp in d2d[2, True, q]:
            cp.wait_recv()
        lax.fori_loop(q * CN // NT, (q + 1) * CN // NT, last, 0)
    closed = {id(cp) for cp in done}
    for cp in open_sends:
        if id(cp) not in closed:
            cp.wait_send()


def per_device(tokens, ln_gain, weights, grad_partials):
    gain = ln_gain.reshape(1, FEAT)
    hbm = pl.BlockSpec(memory_space=pltpu.HBM)
    return pl.pallas_call(
        kernel,
        out_shape=(
            pltpu.VMEM((TOK, COLS), BF16),
            pltpu.VMEM((BLK, COLS), BF16),
        ),
        in_specs=[hbm] * 4,
        out_specs=(pl.BlockSpec(memory_space=pltpu.VMEM),) * 2,
        scratch_shapes=[
            pltpu.VMEM((8, 2 * BLK, COLS), BF16),
            pltpu.VMEM((2, 2, 3, SA // 2, COLS), BF16),
            pltpu.VMEM((2, 3, SB // 2, COLS), BF16),
            pltpu.VMEM((2, SA // 2, COLS), BF16),
            pltpu.VMEM((4, SB, COLS), BF16),
            pltpu.VMEM((NMP, TOK, FEAT), BF16),
            pltpu.VMEM((NMP, 1, FEAT), BF16),
            pltpu.VMEM((BLK, COLS), F32),
            pltpu.VMEM((BLK, COLS), BF16),
            pltpu.VMEM((TOK, COLS), F32),
            pltpu.VMEM((2, 8, 128), F32),
            pltpu.VMEM((22, 8, 128), F32),
            pltpu.SemaphoreType.DMA((NSEM,)),
            pltpu.SemaphoreType.DMA((NSEM,)),
            pltpu.SemaphoreType.DMA((16,)),
        ],
        compiler_params=pltpu.CompilerParams(
            collective_id=0, has_side_effects=True, vmem_limit_bytes=50 * 1024 * 1024
        ),
    )(tokens, gain, weights, grad_partials)


def solution(mesh):
    torus = Mesh(mesh.devices.reshape(4, 2, 2, 2, 4), AXES)
    placed = (P(DP, MP), P(MP), P(DP, MP), P(DP, None, MP))
    return jax.shard_map(
        per_device, mesh=torus, in_specs=placed, out_specs=(P(DP, MP), P(DP, MP)), check_vma=False
    )
```

```python
import functools
import math

import jax
import jax.numpy as jnp
from jax import lax
from jax.experimental import pallas as pl
from jax.experimental.pallas import tpu as pltpu
from jax.sharding import Mesh
from jax.sharding import PartitionSpec as P

FF = 12288
MP = ("mp_0", "mp_1")
DP = ("dp_0", "dp_1", "dp_2")
AXES = ("dp_0", "dp_1", "dp_2", "mp_0", "mp_1")
MESH = pl.DeviceIdType.MESH

BLK = 384
COLS = 1536
TOK = 768
FEAT = 768
NMP = 8
D = FEAT * NMP
SA = 288
SB = BLK - SA
GA = 224
GB = BLK - GA
CH = 16
NT = 256
NSEM = 52
GPAD = 1024
F32 = jnp.float32
BF16 = jnp.bfloat16
R, L = 0, 1


def kernel(
    tok_hbm, gain_hbm, w_hbm, grad_hbm, hid, pert,
    pb, xa, xb, ya, yb, tok, gb, gf, wb, pre, nsend, nrecv,
    ssem, rsem, lsem,
):
    x, yh, c, yl, z = [lax.axis_index(a) for a in AXES]
    y = yh * 2 + yl

    def xid(k):
        return {"dp_0": lax.rem(x + k, 4)}

    def yid(k):
        yy = lax.rem(y + k, 4)
        return {"dp_1": yy // 2, "mp_0": lax.rem(yy, 2)}

    def zid(k):
        return {"mp_1": lax.rem(z + k, 4)}

    core = {"dp_2": 1 - c}
    ypair = {"mp_0": 1 - yl}
    yfar = {"dp_1": 1 - yh}
    xdev = (xid(1), xid(3))

    count = {"s": 0, "l": 0}
    open_sends = []
    closed = set()
    again = []
    slot_of = {}

    def send(src, dst, dev, at=None):
        if at is None:
            at = again.pop() if again else count["s"]
            if at == count["s"]:
                count["s"] += 1
        i = at
        cp = pltpu.make_async_remote_copy(
            src_ref=src, dst_ref=dst, send_sem=ssem.at[i], recv_sem=rsem.at[i],
            device_id=dev, device_id_type=MESH,
        )
        cp.start()
        open_sends.append(cp)
        slot_of[id(cp)] = i
        return cp

    def group(src, dsts, devs):
        at = count["s"]
        count["s"] += 1
        for dst, dev in zip(dsts, devs):
            closed.add(id(send(src, dst, dev, at)))
        return at

    def group_wait(at, ref):
        cp = pltpu.make_async_remote_copy(
            src_ref=ref, dst_ref=ref, send_sem=ssem.at[at], recv_sem=rsem.at[at],
            device_id=core, device_id_type=MESH,
        )
        cp.wait_recv()
        cp.wait_send()

    def flush(cps):
        for cp in cps:
            if id(cp) not in closed:
                closed.add(id(cp))
                cp.wait_send()

    def local(src, dst):
        i = count["l"]
        count["l"] += 1
        cp = pltpu.make_async_copy(src, dst, lsem.at[i])
        cp.start()
        return cp

    def rows(start, n):
        return pl.ds(pl.multiple_of(start, 16), n)

    mine0 = c * BLK
    peer0 = (1 - c) * BLK
    peer_dst = c * BLK

    def block(xk, far):
        return lax.rem(x + xk, 4) * 2 + ((1 - yh) if far else yh)

    def own(j, r0, n):
        return pb.at[j, rows(mine0 + r0, n), :]

    barrier = pltpu.get_barrier_semaphore()
    chips = [core, *(xid(k) for k in (1, 2, 3)), *({**xid(k), **core} for k in (1, 2, 3))]
    planes = [{**yid(i), **zid(k)} for i in range(4) for k in range(4) if i or k]
    peers = chips + planes
    for p in peers:
        pl.semaphore_signal(barrier, inc=1, device_id=p, device_id_type=MESH)
    order = [(2, True), (1, True), (3, True), (0, True), (2, False), (1, False), (3, False), (0, False)]
    mine = {}
    for key in order:
        j = block(*key)
        mine[key] = local(grad_hbm.at[0, rows(2 * j * BLK + mine0, BLK), :], own(j, 0, BLK))
    me_t, pa_t = yl * 4 + z, (1 - yl) * 4 + z
    def gains(k):
        return gb.at[pl.ds(pl.multiple_of(k * GPAD, GPAD), FEAT)]

    lt = local(tok_hbm, tok.at[me_t])
    lg = local(gain_hbm, gains(me_t))
    lw = local(w_hbm, wb)
    pl.semaphore_wait(barrier, len(peers))

    theirs = {}
    HA, HB = SA // 2, SB // 2
    for key in order:
        j = block(*key)
        cuts = (0, HA, SA, BLK) if key == order[0] else (0, BLK)
        theirs[key] = [
            send(grad_hbm.at[0, rows(2 * j * BLK + peer0 + lo, hi - lo), :], pb.at[j, rows(peer_dst + lo, hi - lo), :], core)
            for lo, hi in zip(cuts, cuts[1:])
        ]
    ty = send(tok_hbm, tok.at[me_t], ypair)
    t1 = [send(tok_hbm, tok.at[me_t], zid(k)) for k in (1, 3)]
    gy = send(gain_hbm, gains(me_t), ypair)
    g1 = group(gain_hbm, [gains(me_t)] * 3, [zid(k) for k in (1, 2, 3)])

    def add(j, r0, n, extra=()):
        def body(i, _):
            r = rows(mine0 + r0 + i * CH, CH)
            v = pb[j, r, :].astype(F32) + pb[j, rows(peer0 + r0 + i * CH, CH), :].astype(F32)
            for ref, base in extra:
                v = v + ref[rows(base + i * CH, CH), :].astype(F32)
            pb[j, r, :] = v.astype(BF16)
            return 0

        lax.fori_loop(0, n // CH, body, 0)

    def ready(key, first=0):
        if not first:
            mine[key].wait()
        theirs[key][first].wait_recv()
        return block(*key)

    def a_send(j, near, half, d, slot):
        return send(own(j, half * HA, HA), xa.at[d, near, slot], xdev[d])

    def b_send(j, half, d, slot):
        return send(own(j, SA + half * HB, HB), xb.at[d, slot], xdev[d])

    rs = []

    def y_send(key):
        j = block(*key)
        xx = lax.rem(x + key[0], 4)
        add(j, SA, SB)
        cp = send(own(j, SA, SB), yb.at[xx], yfar)
        rs.append(cp)
        return cp

    def a_open(far):
        near = 0 if far else 1
        j = ready((2, far))
        add(j, 0, HA)
        r0 = a_send(j, near, 0, R, 0)
        if far:
            ready((2, far), 1)
        add(j, HA, HA)
        l0 = a_send(j, near, 1, L, 0)
        j = ready((1, far))
        add(j, HA, HA)
        r1 = a_send(j, near, 1, R, 2)
        j = ready((3, far))
        add(j, 0, HA)
        l1 = a_send(j, near, 0, L, 1)
        rs.extend((r0, l0, r1, l1))
        return r0, l0, r1, l1

    def a_pass(far, opened):
        near = 0 if far else 1
        r0, l0, r1, l1 = opened
        jr, jl = block(1, far), block(3, far)
        r0.wait_recv()
        add(jr, 0, HA, [(xa.at[R, near, 0], 0)])
        r2 = a_send(jr, near, 0, R, 1)
        l0.wait_recv()
        add(jl, HA, HA, [(xa.at[L, near, 0], 0)])
        l2 = a_send(jl, near, 1, L, 2)
        rs.extend((r2, l2))
        return r1, r2, l1, l2

    far_a = a_open(True)
    yrb = {}
    ready((2, True), 2)
    for xk in (2, 1, 3):
        yrb[xk] = y_send((xk, True))
    ready((0, True))
    yrb[0] = y_send((0, True))
    far_a = a_pass(True, far_a)
    near_a = a_open(False)

    for cp in t1:
        cp.wait_recv()
    TH = TOK // 2
    left_t, right_t = lax.rem(z + 3, 4), lax.rem(z + 1, 4)

    def pass_tokens(base):
        lo = send(tok.at[base + left_t, pl.ds(0, TH), :], tok.at[base + left_t, pl.ds(0, TH), :], zid(1))
        hi = send(tok.at[base + right_t, pl.ds(TH, TH), :], tok.at[base + right_t, pl.ds(TH, TH), :], zid(3))
        return [lo, hi]

    t2 = pass_tokens(yl * 4)

    jf = block(0, True)
    for cp in far_a:
        cp.wait_recv()
    yra = []
    for h in range(2):
        add(jf, h * HA, HA, [(xa.at[R, 0, 1 + h], 0), (xa.at[L, 0, 1 + h], 0)])
        yra.append(send(own(jf, h * HA, HA), ya.at[h], yfar))
    rs += yra

    ty.wait_recv()
    gy.wait_recv()
    t3 = [send(tok.at[pa_t], tok.at[pa_t], zid(k)) for k in (1, 3)]
    g3 = group(gains(pa_t), [gains(pa_t)] * 3, [zid(k) for k in (1, 2, 3)])

    near_a = a_pass(False, near_a)
    early = list(rs)

    def b_add(key, half, extra=()):
        j = block(*key)
        xx = lax.rem(x + key[0], 4)
        add(j, SA + half * HB, HB, [(yb.at[xx], half * HB), *extra])
        return j

    yrb[2].wait_recv()
    br0 = b_send(b_add((2, False), 0), 0, R, 0)
    bl0 = b_send(b_add((2, False), 1), 1, L, 0)
    yrb[1].wait_recv()
    br1 = b_send(b_add((1, False), 1), 1, R, 2)
    yrb[3].wait_recv()
    bl1 = b_send(b_add((3, False), 0), 0, L, 1)
    br0.wait_recv()
    br2 = b_send(b_add((1, False), 0, [(xb.at[R, 0], 0)]), 0, R, 1)
    bl0.wait_recv()
    bl2 = b_send(b_add((3, False), 1, [(xb.at[L, 0], 0)]), 1, L, 2)
    rs += [br0, bl0, br1, bl1, br2, bl2]

    jo = ready((0, False))

    def finish(r0, n, extra, acc):
        def body(i, a):
            rh = rows(r0 + i * CH, CH)
            v = pb[jo, rows(mine0 + r0 + i * CH, CH), :].astype(F32) + pb[jo, rows(peer0 + r0 + i * CH, CH), :].astype(F32)
            for ref, base in extra:
                v = v + ref[rows(base + i * CH, CH), :].astype(F32)
            gf[rh, :] = v
            s = v * v
            s = s[:8] + s[8:]
            t = s[:, :128]
            for k in range(1, COLS // 128):
                t = t + s[:, k * 128:(k + 1) * 128]
            return a + t

        return lax.fori_loop(0, n // CH, body, acc)

    acc = jnp.zeros((8, 128), F32)
    phase = [*early, *(cp for cps in theirs.values() for cp in cps), ty, gy, *t1]
    flush(phase)
    for cp in [*near_a, *yra]:
        cp.wait_recv()
    for h in range(2):
        acc = finish(h * HA, HA, [(xa.at[R, 1, 1 + h], 0), (xa.at[L, 1, 1 + h], 0), (ya.at[h], 0)], acc)
    yrb[0].wait_recv()
    for cp in (br1, bl1, br2, bl2):
        cp.wait_recv()
    for h in range(2):
        acc = finish(SA + h * HB, HB, [(yb.at[x], h * HB), (xb.at[R, 1 + h], 0), (xb.at[L, 1 + h], 0)], acc)
    flush(rs)
    phase += [cp for cp in rs if id(cp) not in {id(e) for e in early}]

    slot = 0
    for stage, devs in enumerate((chips, planes)):
        nsend[stage] = acc
        n = len(devs)
        at = group(nsend.at[stage], [nrecv.at[slot + k] for k in range(n)], devs)
        if stage == 1:
            for cp in t3:
                cp.wait_recv()
            t4 = pass_tokens((1 - yl) * 4)
        group_wait(at, nrecv.at[pl.ds(slot, n)])
        for k in range(n):
            acc = acc + nrecv[slot + k]
        slot += n
    squares = jnp.sum(jnp.sum(acc, axis=0, keepdims=True), axis=1, keepdims=True)
    scale = 0.7 * math.sqrt(FF) / jnp.sqrt(squares + 1e-12)

    again += sorted((slot_of[id(cp)] for cp in phase), reverse=True)

    lw.wait()

    def perturb(i, _):
        r = rows(i * CH, CH)
        v = (wb[r, :].astype(F32) + scale * gf[r, :]).astype(BF16)
        pb[jo, rows(mine0 + i * CH, CH), :] = v
        pert[r, :] = v
        return 0

    PA, PB = GA // 2, GB // 2

    def go(j, r0, n, dev, c0=0, cn=COLS):
        ref = pb.at[j, rows(mine0 + r0, n), pl.ds(c0, cn)]
        return send(ref, ref, dev)

    d2d = {}

    def across(xk, far, r0, n, part=0, c0=0, cn=COLS):
        j = block(xk, far)
        d2d.setdefault((xk, far, part), []).append(go(j, r0, n, core, c0, cn))

    lax.fori_loop(GA // CH, BLK // CH, perturb, 0)
    ob = [go(jo, GA, GB, xdev[d]) for d in (R, L)]
    lax.fori_loop(0, GA // CH, perturb, 0)
    ya1 = go(jo, 0, GA, yfar)
    oa = [go(jo, 0, GA, xdev[d]) for d in (R, L)]
    across(0, False, 0, BLK)
    yb1 = go(jo, GA, GB, yfar)

    old = list(open_sends)

    ob[R].wait_recv()
    yl_b = go(block(3, False), GA, GB, yfar)
    across(3, False, GA, GB)
    ob[L].wait_recv()
    yr_b = go(block(1, False), GA, GB, yfar)
    across(1, False, GA, GB)
    ya1.wait_recv()
    fra = [go(block(0, True), 0, GA, xdev[d]) for d in (R, L)]
    fb = [go(block(3, False), GA, PB, xdev[R]), go(block(1, False), GA + PB, PB, xdev[L])]
    across(0, True, 0, GA)

    lt.wait()
    lg.wait()
    for cp in [*t2, *t4]:
        cp.wait_recv()
    for at in (g1, g3):
        group_wait(at, gb.at[pl.ds(0, 3 * FEAT)])
    flush([*t2, *t3, *t4])

    def norm_rows(i, _):
        r = rows(i * CH, CH)
        tot = tok[0, r, :].astype(F32)
        for k in range(1, NMP):
            tot = tot + tok[k, r, :].astype(F32)
        mean = jnp.sum(tot, axis=1, keepdims=True) * (1.0 / D)
        dev = None
        for k in range(NMP):
            e = tok[k, r, :].astype(F32) - mean
            dev = e * e if dev is None else dev + e * e
        var = jnp.sum(dev, axis=1, keepdims=True) * (1.0 / D)
        inv = 1.0 / jnp.sqrt(var + 1e-6)
        for k in range(NMP):
            e = (tok[k, r, :].astype(F32) - mean) * inv * gb[pl.ds(k * GPAD, FEAT)].astype(F32).reshape(1, FEAT)
            tok[k, r, :] = e.astype(BF16)
        return 0

    lax.fori_loop(0, TOK // CH, norm_rows, 0)

    def dots(j, n):
        cols = pl.ds(pl.multiple_of(n * NT, NT), NT)
        return jnp.dot(tok[j], pb[j, :, cols], preferred_element_type=F32)

    def multiply(xk, far, first=False, lo=0, hi=COLS):
        j = block(xk, far)
        if lo == 0:
            for cp in d2d[xk, far, 0]:
                cp.wait_recv()

        def body(n, _):
            cols = pl.ds(pl.multiple_of(n * NT, NT), NT)
            if first:
                pre[:, cols] = dots(j, n)
            else:
                pre[:, cols] = pre[:, cols] + dots(j, n)
            return 0

        lax.fori_loop(lo // NT, hi // NT, body, 0, unroll=3)

    oa[R].wait_recv()
    fa = [go(block(3, False), 0, PA, xdev[R])]
    across(3, False, 0, GA)
    oa[L].wait_recv()
    fa.append(go(block(1, False), PA, PA, xdev[L]))
    across(1, False, 0, GA)
    yb1.wait_recv()
    across(0, True, GA, GB)
    multiply(0, False, True)
    multiply(0, True)
    multiply(3, False)
    multiply(1, False)
    flush(old)
    CN = 2 * COLS // 3
    cuts = ((0, CN), (CN, COLS - CN))
    fra[R].wait_recv()
    ffa = [[go(block(3, True), 0, PA, xdev[R], *q) for q in cuts]]
    across(3, True, 0, GA)
    fra[L].wait_recv()
    ffa.append([go(block(1, True), PA, PA, xdev[L], *q) for q in cuts])
    across(1, True, 0, GA)
    y2 = []
    for k in range(2):
        fb[k].wait_recv()
        y2.append(go(block(2, False), GA + k * PB, PB, yfar))
        across(2, False, GA + k * PB, PB)
    yl_b.wait_recv()
    across(3, True, GA, GB)
    yr_b.wait_recv()
    across(1, True, GA, GB)
    multiply(3, True)
    multiply(1, True)
    for k in range(2):
        fa[k].wait_recv()
        across(2, False, k * PA, PA)
    older = [*fra, *fb, yl_b, yr_b, *fa, *d2d[3, True, 0], *d2d[1, True, 0], *d2d[2, False, 0]]
    multiply(2, False, False, 0, COLS // 2)
    for k in range(2):
        y2[k].wait_recv()
        across(2, True, GA + k * PB, PB)
    for k in range(2):
        ffa[k][0].wait_recv()
        across(2, True, k * PA, PA, 0, *cuts[0])
    multiply(2, False, False, COLS // 2, COLS)
    flush(older)
    jl = block(2, True)

    def last(n, _):
        cols = pl.ds(pl.multiple_of(n * NT, NT), NT)
        v = pre[:, cols] + dots(jl, n)
        hid[:, cols] = (v * 0.5 * (1.0 + lax.erf(v * (1.0 / math.sqrt(2.0))))).astype(BF16)
        return 0

    def finish_columns(lo, hi):
        lax.fori_loop(lo // NT, hi // NT, last, 0, unroll=2)

    for cp in d2d[2, True, 0]:
        cp.wait_recv()
    finish_columns(0, CN // 2)
    for k in range(2):
        ffa[k][1].wait_recv()
        across(2, True, k * PA, PA, 1, *cuts[1])
    finish_columns(CN // 2, CN)
    for cp in d2d[2, True, 1]:
        cp.wait_recv()
    finish_columns(CN, COLS)
    flush(open_sends)
    assert count["s"] <= NSEM and count["l"] == 11, count


def per_device(tokens, ln_gain, weights, grad_partials):
    hbm = pl.BlockSpec(memory_space=pltpu.HBM)
    return pl.pallas_call(
        kernel,
        out_shape=(
            pltpu.VMEM((TOK, COLS), BF16),
            pltpu.VMEM((BLK, COLS), BF16),
        ),
        in_specs=[hbm] * 4,
        out_specs=(pl.BlockSpec(memory_space=pltpu.VMEM),) * 2,
        scratch_shapes=[
            pltpu.VMEM((8, 2 * BLK, COLS), BF16),
            pltpu.VMEM((2, 2, 3, SA // 2, COLS), BF16),
            pltpu.VMEM((2, 3, SB // 2, COLS), BF16),
            pltpu.VMEM((2, SA // 2, COLS), BF16),
            pltpu.VMEM((4, SB, COLS), BF16),
            pltpu.VMEM((NMP, TOK, FEAT), BF16),
            pltpu.VMEM((NMP * GPAD,), BF16),
            pltpu.VMEM((BLK, COLS), F32),
            pltpu.VMEM((BLK, COLS), BF16),
            pltpu.VMEM((TOK, COLS), F32),
            pltpu.VMEM((2, 8, 128), F32),
            pltpu.VMEM((22, 8, 128), F32),
            pltpu.SemaphoreType.DMA((NSEM,)),
            pltpu.SemaphoreType.DMA((NSEM,)),
            pltpu.SemaphoreType.DMA((11,)),
        ],
        compiler_params=pltpu.CompilerParams(
            collective_id=0, has_side_effects=True, vmem_limit_bytes=50 * 1024 * 1024
        ),
    )(tokens, ln_gain, weights, grad_partials)


def solution(mesh):
    torus = Mesh(mesh.devices.reshape(4, 2, 2, 2, 4), AXES)
    placed = (P(DP, MP), P(MP), P(DP, MP), P(DP, None, MP))
    return jax.shard_map(
        per_device, mesh=torus, in_specs=placed, out_specs=(P(DP, MP), P(DP, MP)), check_vma=False
    )
```

```python
import functools
import math

import jax
import jax.numpy as jnp
from jax import lax
from jax.experimental import pallas as pl
from jax.experimental.pallas import tpu as pltpu
from jax.sharding import Mesh
from jax.sharding import PartitionSpec as P

FF = 12288
MP = ("mp_0", "mp_1")
DP = ("dp_0", "dp_1", "dp_2")
AXES = ("dp_0", "dp_1", "dp_2", "mp_0", "mp_1")
MESH = pl.DeviceIdType.MESH

BLK = 384
COLS = 1536
TOK = 768
FEAT = 768
NMP = 8
D = FEAT * NMP
SA = 288
SB = BLK - SA
GA = 224
GB = BLK - GA
CH = 16
NT = 256
NSEM = 52
GPAD = 1024
F32 = jnp.float32
BF16 = jnp.bfloat16
R, L = 0, 1


def kernel(
    tok_hbm, gain_hbm, w_hbm, grad_hbm, hid, pert,
    pb, xa, xb, ya, yb, tok, gb, gf, wb, pre, nsend, nrecv,
    ssem, rsem, lsem,
):
    x, yh, c, yl, z = [lax.axis_index(a) for a in AXES]
    y = yh * 2 + yl

    def xid(k):
        return {"dp_0": lax.rem(x + k, 4)}

    def yid(k):
        yy = lax.rem(y + k, 4)
        return {"dp_1": yy // 2, "mp_0": lax.rem(yy, 2)}

    def zid(k):
        return {"mp_1": lax.rem(z + k, 4)}

    core = {"dp_2": 1 - c}
    ypair = {"mp_0": 1 - yl}
    yfar = {"dp_1": 1 - yh}
    xdev = (xid(1), xid(3))

    count = {"s": 0, "l": 0}
    open_sends = []
    closed = set()
    again = []
    slot_of = {}

    def send(src, dst, dev, at=None):
        if at is None:
            at = again.pop() if again else count["s"]
            if at == count["s"]:
                count["s"] += 1
        i = at
        cp = pltpu.make_async_remote_copy(
            src_ref=src, dst_ref=dst, send_sem=ssem.at[i], recv_sem=rsem.at[i],
            device_id=dev, device_id_type=MESH,
        )
        cp.start()
        open_sends.append(cp)
        slot_of[id(cp)] = i
        return cp

    def group(src, dsts, devs):
        at = count["s"]
        count["s"] += 1
        for dst, dev in zip(dsts, devs):
            closed.add(id(send(src, dst, dev, at)))
        return at

    def group_wait(at, ref):
        cp = pltpu.make_async_remote_copy(
            src_ref=ref, dst_ref=ref, send_sem=ssem.at[at], recv_sem=rsem.at[at],
            device_id=core, device_id_type=MESH,
        )
        cp.wait_recv()
        cp.wait_send()

    def flush(cps):
        for cp in cps:
            if id(cp) not in closed:
                closed.add(id(cp))
                cp.wait_send()

    def local(src, dst):
        i = count["l"]
        count["l"] += 1
        cp = pltpu.make_async_copy(src, dst, lsem.at[i])
        cp.start()
        return cp

    def rows(start, n):
        return pl.ds(pl.multiple_of(start, 16), n)

    mine0 = c * BLK
    peer0 = (1 - c) * BLK
    peer_dst = c * BLK

    def block(xk, far):
        return lax.rem(x + xk, 4) * 2 + ((1 - yh) if far else yh)

    def own(j, r0, n):
        return pb.at[j, rows(mine0 + r0, n), :]

    barrier = pltpu.get_barrier_semaphore()
    chips = [core, *(xid(k) for k in (1, 2, 3)), *({**xid(k), **core} for k in (1, 2, 3))]
    planes = [{**yid(i), **zid(k)} for i in range(4) for k in range(4) if i or k]
    peers = chips + planes
    for p in peers:
        pl.semaphore_signal(barrier, inc=1, device_id=p, device_id_type=MESH)
    order = [(2, True), (1, True), (3, True), (0, True), (2, False), (1, False), (3, False), (0, False)]
    mine = {}
    for key in order:
        j = block(*key)
        mine[key] = local(grad_hbm.at[0, rows(2 * j * BLK + mine0, BLK), :], own(j, 0, BLK))
    me_t, pa_t = yl * 4 + z, (1 - yl) * 4 + z
    def gains(k):
        return gb.at[pl.ds(pl.multiple_of(k * GPAD, GPAD), FEAT)]

    lt = local(tok_hbm, tok.at[me_t])
    lg = local(gain_hbm, gains(me_t))
    lw = local(w_hbm, wb)
    pl.semaphore_wait(barrier, len(peers))

    theirs = {}
    HA, HB = SA // 2, SB // 2
    for key in order:
        j = block(*key)
        cuts = (0, HA, SA, BLK) if key == order[0] else (0, BLK)
        theirs[key] = [
            send(grad_hbm.at[0, rows(2 * j * BLK + peer0 + lo, hi - lo), :], pb.at[j, rows(peer_dst + lo, hi - lo), :], core)
            for lo, hi in zip(cuts, cuts[1:])
        ]
    ty = send(tok_hbm, tok.at[me_t], ypair)
    t1 = [send(tok_hbm, tok.at[me_t], zid(k)) for k in (1, 3)]
    gy = send(gain_hbm, gains(me_t), ypair)
    g1 = group(gain_hbm, [gains(me_t)] * 3, [zid(k) for k in (1, 2, 3)])

    def add(j, r0, n, extra=()):
        def body(i, _):
            r = rows(mine0 + r0 + i * CH, CH)
            v = pb[j, r, :].astype(F32) + pb[j, rows(peer0 + r0 + i * CH, CH), :].astype(F32)
            for ref, base in extra:
                v = v + ref[rows(base + i * CH, CH), :].astype(F32)
            pb[j, r, :] = v.astype(BF16)
            return 0

        lax.fori_loop(0, n // CH, body, 0)

    def ready(key, first=0):
        if not first:
            mine[key].wait()
        theirs[key][first].wait_recv()
        return block(*key)

    def a_send(j, near, half, d, slot):
        return send(own(j, half * HA, HA), xa.at[d, near, slot], xdev[d])

    def b_send(j, half, d, slot):
        return send(own(j, SA + half * HB, HB), xb.at[d, slot], xdev[d])

    rs = []

    def y_send(key):
        j = block(*key)
        xx = lax.rem(x + key[0], 4)
        add(j, SA, SB)
        cp = send(own(j, SA, SB), yb.at[xx], yfar)
        rs.append(cp)
        return cp

    def a_open(far):
        near = 0 if far else 1
        j = ready((2, far))
        add(j, 0, HA)
        r0 = a_send(j, near, 0, R, 0)
        if far:
            ready((2, far), 1)
        add(j, HA, HA)
        l0 = a_send(j, near, 1, L, 0)
        j = ready((1, far))
        add(j, HA, HA)
        r1 = a_send(j, near, 1, R, 2)
        j = ready((3, far))
        add(j, 0, HA)
        l1 = a_send(j, near, 0, L, 1)
        rs.extend((r0, l0, r1, l1))
        return r0, l0, r1, l1

    def a_pass(far, opened):
        near = 0 if far else 1
        r0, l0, r1, l1 = opened
        jr, jl = block(1, far), block(3, far)
        r0.wait_recv()
        add(jr, 0, HA, [(xa.at[R, near, 0], 0)])
        r2 = a_send(jr, near, 0, R, 1)
        l0.wait_recv()
        add(jl, HA, HA, [(xa.at[L, near, 0], 0)])
        l2 = a_send(jl, near, 1, L, 2)
        rs.extend((r2, l2))
        return r1, r2, l1, l2

    far_a = a_open(True)
    yrb = {}
    ready((2, True), 2)
    for xk in (2, 1, 3):
        yrb[xk] = y_send((xk, True))
    ready((0, True))
    yrb[0] = y_send((0, True))
    far_a = a_pass(True, far_a)
    near_a = a_open(False)

    for cp in t1:
        cp.wait_recv()
    TH = TOK // 2
    left_t, right_t = lax.rem(z + 3, 4), lax.rem(z + 1, 4)

    def pass_tokens(base):
        lo = send(tok.at[base + left_t, pl.ds(0, TH), :], tok.at[base + left_t, pl.ds(0, TH), :], zid(1))
        hi = send(tok.at[base + right_t, pl.ds(TH, TH), :], tok.at[base + right_t, pl.ds(TH, TH), :], zid(3))
        return [lo, hi]

    t2 = pass_tokens(yl * 4)

    jf = block(0, True)
    for cp in far_a:
        cp.wait_recv()
    yra = []
    for h in range(2):
        add(jf, h * HA, HA, [(xa.at[R, 0, 1 + h], 0), (xa.at[L, 0, 1 + h], 0)])
        yra.append(send(own(jf, h * HA, HA), ya.at[h], yfar))
    rs += yra

    ty.wait_recv()
    gy.wait_recv()
    t3 = [send(tok.at[pa_t], tok.at[pa_t], zid(k)) for k in (1, 3)]
    g3 = group(gains(pa_t), [gains(pa_t)] * 3, [zid(k) for k in (1, 2, 3)])

    near_a = a_pass(False, near_a)
    early = list(rs)

    def b_add(key, half, extra=()):
        j = block(*key)
        xx = lax.rem(x + key[0], 4)
        add(j, SA + half * HB, HB, [(yb.at[xx], half * HB), *extra])
        return j

    yrb[2].wait_recv()
    br0 = b_send(b_add((2, False), 0), 0, R, 0)
    bl0 = b_send(b_add((2, False), 1), 1, L, 0)
    yrb[1].wait_recv()
    br1 = b_send(b_add((1, False), 1), 1, R, 2)
    yrb[3].wait_recv()
    bl1 = b_send(b_add((3, False), 0), 0, L, 1)
    br0.wait_recv()
    br2 = b_send(b_add((1, False), 0, [(xb.at[R, 0], 0)]), 0, R, 1)
    bl0.wait_recv()
    bl2 = b_send(b_add((3, False), 1, [(xb.at[L, 0], 0)]), 1, L, 2)
    rs += [br0, bl0, br1, bl1, br2, bl2]

    jo = ready((0, False))

    def terms(r0, i, extra):
        v = pb[jo, rows(mine0 + r0 + i * CH, CH), :].astype(F32)
        v = v + pb[jo, rows(peer0 + r0 + i * CH, CH), :].astype(F32)
        for ref, base in extra:
            v = v + ref[rows(base + i * CH, CH), :].astype(F32)
        return v

    def squared(v):
        s = v * v
        s = s[:8] + s[8:]
        t = s[:, :128]
        for k in range(1, COLS // 128):
            t = t + s[:, k * 128:(k + 1) * 128]
        return t

    def gather_terms(r0, n, extra):
        def body(i, _):
            gf[rows(r0 + i * CH, CH), :] = terms(r0, i, extra)
            return 0

        lax.fori_loop(0, n // CH, body, 0)

    def finish(r0, n, extra, acc):
        def body(i, a):
            v = terms(r0, i, extra)
            gf[rows(r0 + i * CH, CH), :] = v
            return a + squared(v)

        return lax.fori_loop(0, n // CH, body, acc)

    def finish_last(r0, n, ref, acc):
        def body(i, a):
            r = rows(r0 + i * CH, CH)
            v = gf[r, :] + ref[rows(i * CH, CH), :].astype(F32)
            gf[r, :] = v
            return a + squared(v)

        return lax.fori_loop(0, n // CH, body, acc)

    acc = jnp.zeros((8, 128), F32)
    phase = [*early, *(cp for cps in theirs.values() for cp in cps), ty, gy, *t1]
    for cp in near_a:
        cp.wait_recv()
    for h in range(2):
        gather_terms(h * HA, HA, [(xa.at[R, 1, 1 + h], 0), (xa.at[L, 1, 1 + h], 0)])
    flush(phase)
    yrb[0].wait_recv()
    for cp in (br1, bl1, br2, bl2):
        cp.wait_recv()
    for h in range(2):
        acc = finish(SA + h * HB, HB, [(yb.at[x], h * HB), (xb.at[R, 1 + h], 0), (xb.at[L, 1 + h], 0)], acc)
    for h in range(2):
        yra[h].wait_recv()
        acc = finish_last(h * HA, HA, ya.at[h], acc)
    flush(rs)
    phase += [cp for cp in rs if id(cp) not in {id(e) for e in early}]

    slot = 0
    for stage, devs in enumerate((chips, planes)):
        nsend[stage] = acc
        n = len(devs)
        at = group(nsend.at[stage], [nrecv.at[slot + k] for k in range(n)], devs)
        if stage == 1:
            for cp in t3:
                cp.wait_recv()
            t4 = pass_tokens((1 - yl) * 4)
        group_wait(at, nrecv.at[pl.ds(slot, n)])
        for k in range(n):
            acc = acc + nrecv[slot + k]
        slot += n
    squares = jnp.sum(jnp.sum(acc, axis=0, keepdims=True), axis=1, keepdims=True)
    scale = 0.7 * math.sqrt(FF) / jnp.sqrt(squares + 1e-12)

    again += sorted((slot_of[id(cp)] for cp in phase), reverse=True)

    lw.wait()

    def perturb(i, _):
        r = rows(i * CH, CH)
        v = (wb[r, :].astype(F32) + scale * gf[r, :]).astype(BF16)
        pb[jo, rows(mine0 + i * CH, CH), :] = v
        pert[r, :] = v
        return 0

    PA, PB = GA // 2, GB // 2

    def go(j, r0, n, dev, c0=0, cn=COLS):
        ref = pb.at[j, rows(mine0 + r0, n), pl.ds(c0, cn)]
        return send(ref, ref, dev)

    d2d = {}

    def across(xk, far, r0, n, part=0, c0=0, cn=COLS):
        j = block(xk, far)
        d2d.setdefault((xk, far, part), []).append(go(j, r0, n, core, c0, cn))

    lax.fori_loop(GA // CH, BLK // CH, perturb, 0)
    ob = [go(jo, GA, GB, xdev[d]) for d in (R, L)]
    lax.fori_loop(0, GA // CH, perturb, 0)
    ya1 = go(jo, 0, GA, yfar)
    oa = [go(jo, 0, GA, xdev[d]) for d in (R, L)]
    across(0, False, 0, BLK)
    yb1 = go(jo, GA, GB, yfar)

    old = list(open_sends)

    ob[R].wait_recv()
    yl_b = go(block(3, False), GA, GB, yfar)
    across(3, False, GA, GB)
    ob[L].wait_recv()
    yr_b = go(block(1, False), GA, GB, yfar)
    across(1, False, GA, GB)
    ya1.wait_recv()
    fra = [go(block(0, True), 0, GA, xdev[d]) for d in (R, L)]
    fb = [go(block(3, False), GA, PB, xdev[R]), go(block(1, False), GA + PB, PB, xdev[L])]
    across(0, True, 0, GA)

    lt.wait()
    lg.wait()
    for cp in [*t2, *t4]:
        cp.wait_recv()
    for at in (g1, g3):
        group_wait(at, gb.at[pl.ds(0, 3 * FEAT)])
    flush([*t2, *t3, *t4])

    def norm_rows(i, _):
        r = rows(i * CH, CH)
        tot = tok[0, r, :].astype(F32)
        for k in range(1, NMP):
            tot = tot + tok[k, r, :].astype(F32)
        mean = jnp.sum(tot, axis=1, keepdims=True) * (1.0 / D)
        dev = None
        for k in range(NMP):
            e = tok[k, r, :].astype(F32) - mean
            dev = e * e if dev is None else dev + e * e
        var = jnp.sum(dev, axis=1, keepdims=True) * (1.0 / D)
        inv = 1.0 / jnp.sqrt(var + 1e-6)
        for k in range(NMP):
            e = (tok[k, r, :].astype(F32) - mean) * inv * gb[pl.ds(k * GPAD, FEAT)].astype(F32).reshape(1, FEAT)
            tok[k, r, :] = e.astype(BF16)
        return 0

    lax.fori_loop(0, TOK // CH, norm_rows, 0)

    def dots(j, n):
        cols = pl.ds(pl.multiple_of(n * NT, NT), NT)
        return jnp.dot(tok[j], pb[j, :, cols], preferred_element_type=F32)

    def multiply(xk, far, first=False, lo=0, hi=COLS):
        j = block(xk, far)
        if lo == 0:
            for cp in d2d[xk, far, 0]:
                cp.wait_recv()

        def body(n, _):
            cols = pl.ds(pl.multiple_of(n * NT, NT), NT)
            if first:
                pre[:, cols] = dots(j, n)
            else:
                pre[:, cols] = pre[:, cols] + dots(j, n)
            return 0

        lax.fori_loop(lo // NT, hi // NT, body, 0, unroll=3)

    oa[R].wait_recv()
    fa = [go(block(3, False), 0, PA, xdev[R])]
    across(3, False, 0, GA)
    oa[L].wait_recv()
    fa.append(go(block(1, False), PA, PA, xdev[L]))
    across(1, False, 0, GA)
    yb1.wait_recv()
    across(0, True, GA, GB)
    multiply(0, False, True)
    multiply(0, True)
    multiply(3, False)
    multiply(1, False)
    flush(old)
    CN = 2 * COLS // 3
    cuts = ((0, CN), (CN, COLS - CN))
    fra[R].wait_recv()
    ffa = [[go(block(3, True), 0, PA, xdev[R], *q) for q in cuts]]
    across(3, True, 0, GA)
    fra[L].wait_recv()
    ffa.append([go(block(1, True), PA, PA, xdev[L], *q) for q in cuts])
    across(1, True, 0, GA)
    y2 = []
    for k in range(2):
        fb[k].wait_recv()
        y2.append(go(block(2, False), GA + k * PB, PB, yfar))
        across(2, False, GA + k * PB, PB)
    yl_b.wait_recv()
    across(3, True, GA, GB)
    yr_b.wait_recv()
    across(1, True, GA, GB)
    multiply(3, True)
    multiply(1, True)
    for k in range(2):
        fa[k].wait_recv()
        across(2, False, k * PA, PA)
    older = [*fra, *fb, yl_b, yr_b, *fa, *d2d[3, True, 0], *d2d[1, True, 0], *d2d[2, False, 0]]
    multiply(2, False, False, 0, COLS // 2)
    for k in range(2):
        y2[k].wait_recv()
        across(2, True, GA + k * PB, PB)
    for k in range(2):
        ffa[k][0].wait_recv()
        across(2, True, k * PA, PA, 0, *cuts[0])
    multiply(2, False, False, COLS // 2, COLS)
    flush(older)
    jl = block(2, True)

    def last(n, _):
        cols = pl.ds(pl.multiple_of(n * NT, NT), NT)
        v = pre[:, cols] + dots(jl, n)
        hid[:, cols] = (v * 0.5 * (1.0 + lax.erf(v * (1.0 / math.sqrt(2.0))))).astype(BF16)
        return 0

    def finish_columns(lo, hi):
        lax.fori_loop(lo // NT, hi // NT, last, 0, unroll=2)

    for cp in d2d[2, True, 0]:
        cp.wait_recv()
    finish_columns(0, CN // 2)
    for k in range(2):
        ffa[k][1].wait_recv()
        across(2, True, k * PA, PA, 1, *cuts[1])
    finish_columns(CN // 2, CN)
    for cp in d2d[2, True, 1]:
        cp.wait_recv()
    finish_columns(CN, COLS)
    flush(open_sends)
    assert count["s"] <= NSEM and count["l"] == 11, count


def per_device(tokens, ln_gain, weights, grad_partials):
    hbm = pl.BlockSpec(memory_space=pltpu.HBM)
    return pl.pallas_call(
        kernel,
        out_shape=(
            pltpu.VMEM((TOK, COLS), BF16),
            pltpu.VMEM((BLK, COLS), BF16),
        ),
        in_specs=[hbm] * 4,
        out_specs=(pl.BlockSpec(memory_space=pltpu.VMEM),) * 2,
        scratch_shapes=[
            pltpu.VMEM((8, 2 * BLK, COLS), BF16),
            pltpu.VMEM((2, 2, 3, SA // 2, COLS), BF16),
            pltpu.VMEM((2, 3, SB // 2, COLS), BF16),
            pltpu.VMEM((2, SA // 2, COLS), BF16),
            pltpu.VMEM((4, SB, COLS), BF16),
            pltpu.VMEM((NMP, TOK, FEAT), BF16),
            pltpu.VMEM((NMP * GPAD,), BF16),
            pltpu.VMEM((BLK, COLS), F32),
            pltpu.VMEM((BLK, COLS), BF16),
            pltpu.VMEM((TOK, COLS), F32),
            pltpu.VMEM((2, 8, 128), F32),
            pltpu.VMEM((22, 8, 128), F32),
            pltpu.SemaphoreType.DMA((NSEM,)),
            pltpu.SemaphoreType.DMA((NSEM,)),
            pltpu.SemaphoreType.DMA((11,)),
        ],
        compiler_params=pltpu.CompilerParams(
            collective_id=0, has_side_effects=True, vmem_limit_bytes=50 * 1024 * 1024
        ),
    )(tokens, ln_gain, weights, grad_partials)


def solution(mesh):
    torus = Mesh(mesh.devices.reshape(4, 2, 2, 2, 4), AXES)
    placed = (P(DP, MP), P(MP), P(DP, MP), P(DP, None, MP))
    return jax.shard_map(
        per_device, mesh=torus, in_specs=placed, out_specs=(P(DP, MP), P(DP, MP)), check_vma=False
    )
```

```python
import functools
import math

import jax
import jax.numpy as jnp
from jax import lax
from jax.experimental import pallas as pl
from jax.experimental.pallas import tpu as pltpu
from jax.sharding import Mesh
from jax.sharding import PartitionSpec as P

FF = 12288
MP = ("mp_0", "mp_1")
DP = ("dp_0", "dp_1", "dp_2")
AXES = ("dp_0", "dp_1", "dp_2", "mp_0", "mp_1")
MESH = pl.DeviceIdType.MESH

BLK = 384
COLS = 1536
TOK = 768
FEAT = 768
NMP = 8
D = FEAT * NMP
SA = 288
SB = BLK - SA
GA = 224
GB = BLK - GA
CH = 16
NT = 256
NSEM = 52
GPAD = 1024
F32 = jnp.float32
BF16 = jnp.bfloat16
R, L = 0, 1


def kernel(
    tok_hbm, gain_hbm, w_hbm, grad_hbm, hid, pert,
    pb, xa, xb, ya, yb, tok, gb, gf, wb, pre, nsend, nrecv,
    ssem, rsem, lsem,
):
    x, yh, c, yl, z = [lax.axis_index(a) for a in AXES]
    y = yh * 2 + yl

    def xid(k):
        return {"dp_0": lax.rem(x + k, 4)}

    def yid(k):
        yy = lax.rem(y + k, 4)
        return {"dp_1": yy // 2, "mp_0": lax.rem(yy, 2)}

    def zid(k):
        return {"mp_1": lax.rem(z + k, 4)}

    core = {"dp_2": 1 - c}
    ypair = {"mp_0": 1 - yl}
    yfar = {"dp_1": 1 - yh}
    xdev = (xid(1), xid(3))

    count = {"s": 0, "l": 0}
    open_sends = []
    closed = set()
    again = []
    slot_of = {}

    def send(src, dst, dev, at=None):
        if at is None:
            at = again.pop() if again else count["s"]
            if at == count["s"]:
                count["s"] += 1
        i = at
        cp = pltpu.make_async_remote_copy(
            src_ref=src, dst_ref=dst, send_sem=ssem.at[i], recv_sem=rsem.at[i],
            device_id=dev, device_id_type=MESH,
        )
        cp.start()
        open_sends.append(cp)
        slot_of[id(cp)] = i
        return cp

    def group(src, dsts, devs):
        at = count["s"]
        count["s"] += 1
        for dst, dev in zip(dsts, devs):
            closed.add(id(send(src, dst, dev, at)))
        return at

    def group_wait(at, ref):
        cp = pltpu.make_async_remote_copy(
            src_ref=ref, dst_ref=ref, send_sem=ssem.at[at], recv_sem=rsem.at[at],
            device_id=core, device_id_type=MESH,
        )
        cp.wait_recv()
        cp.wait_send()

    def flush(cps):
        for cp in cps:
            if id(cp) not in closed:
                closed.add(id(cp))
                cp.wait_send()

    def local(src, dst):
        i = count["l"]
        count["l"] += 1
        cp = pltpu.make_async_copy(src, dst, lsem.at[i])
        cp.start()
        return cp

    def rows(start, n):
        return pl.ds(pl.multiple_of(start, 16), n)

    mine0 = c * BLK
    peer0 = (1 - c) * BLK
    peer_dst = c * BLK

    def block(xk, far):
        return lax.rem(x + xk, 4) * 2 + ((1 - yh) if far else yh)

    def own(j, r0, n):
        return pb.at[j, rows(mine0 + r0, n), :]

    barrier = pltpu.get_barrier_semaphore()
    chips = [core, *(xid(k) for k in (1, 2, 3)), *({**xid(k), **core} for k in (1, 2, 3))]
    planes = [{**yid(i), **zid(k)} for i in range(4) for k in range(4) if i or k]
    peers = chips + planes
    for p in peers:
        pl.semaphore_signal(barrier, inc=1, device_id=p, device_id_type=MESH)
    order = [(2, True), (1, True), (3, True), (0, True), (2, False), (1, False), (3, False), (0, False)]
    mine = {}
    for key in order:
        j = block(*key)
        mine[key] = local(grad_hbm.at[0, rows(2 * j * BLK + mine0, BLK), :], own(j, 0, BLK))
    me_t, pa_t = yl * 4 + z, (1 - yl) * 4 + z
    def gains(k):
        return gb.at[pl.ds(pl.multiple_of(k * GPAD, GPAD), FEAT)]

    lt = local(tok_hbm, tok.at[me_t])
    lg = local(gain_hbm, gains(me_t))
    lw = local(w_hbm, wb)
    pl.semaphore_wait(barrier, len(peers))

    theirs = {}
    HA, HB = SA // 2, SB // 2
    for key in order:
        j = block(*key)
        cuts = (0, HA, SA, BLK) if key == order[0] else (0, BLK)
        theirs[key] = [
            send(grad_hbm.at[0, rows(2 * j * BLK + peer0 + lo, hi - lo), :], pb.at[j, rows(peer_dst + lo, hi - lo), :], core)
            for lo, hi in zip(cuts, cuts[1:])
        ]
    ty = send(tok_hbm, tok.at[me_t], ypair)
    t1 = [send(tok_hbm, tok.at[me_t], zid(k)) for k in (1, 3)]
    gy = send(gain_hbm, gains(me_t), ypair)
    g1 = group(gain_hbm, [gains(me_t)] * 3, [zid(k) for k in (1, 2, 3)])

    def add(j, r0, n, extra=()):
        def body(i, _):
            r = rows(mine0 + r0 + i * CH, CH)
            v = pb[j, r, :].astype(F32) + pb[j, rows(peer0 + r0 + i * CH, CH), :].astype(F32)
            for ref, base in extra:
                v = v + ref[rows(base + i * CH, CH), :].astype(F32)
            pb[j, r, :] = v.astype(BF16)
            return 0

        lax.fori_loop(0, n // CH, body, 0)

    def ready(key, first=0):
        if not first:
            mine[key].wait()
        theirs[key][first].wait_recv()
        return block(*key)

    def a_send(j, near, half, d, slot):
        return send(own(j, half * HA, HA), xa.at[d, near, slot], xdev[d])

    def b_send(j, half, d, slot):
        return send(own(j, SA + half * HB, HB), xb.at[d, slot], xdev[d])

    rs = []

    def y_send(key):
        j = block(*key)
        xx = lax.rem(x + key[0], 4)
        add(j, SA, SB)
        cp = send(own(j, SA, SB), yb.at[xx], yfar)
        rs.append(cp)
        return cp

    def a_open(far):
        near = 0 if far else 1
        j = ready((2, far))
        add(j, 0, HA)
        r0 = a_send(j, near, 0, R, 0)
        if far:
            ready((2, far), 1)
        add(j, HA, HA)
        l0 = a_send(j, near, 1, L, 0)
        j = ready((1, far))
        add(j, HA, HA)
        r1 = a_send(j, near, 1, R, 2)
        j = ready((3, far))
        add(j, 0, HA)
        l1 = a_send(j, near, 0, L, 1)
        rs.extend((r0, l0, r1, l1))
        return r0, l0, r1, l1

    def a_pass(far, opened):
        near = 0 if far else 1
        r0, l0, r1, l1 = opened
        jr, jl = block(1, far), block(3, far)
        r0.wait_recv()
        add(jr, 0, HA, [(xa.at[R, near, 0], 0)])
        r2 = a_send(jr, near, 0, R, 1)
        l0.wait_recv()
        add(jl, HA, HA, [(xa.at[L, near, 0], 0)])
        l2 = a_send(jl, near, 1, L, 2)
        rs.extend((r2, l2))
        return r1, r2, l1, l2

    far_a = a_open(True)
    yrb = {}
    ready((2, True), 2)
    for xk in (2, 1, 3):
        yrb[xk] = y_send((xk, True))
    ready((0, True))
    yrb[0] = y_send((0, True))
    far_a = a_pass(True, far_a)
    near_a = a_open(False)

    for cp in t1:
        cp.wait_recv()
    TH = TOK // 2
    left_t, right_t = lax.rem(z + 3, 4), lax.rem(z + 1, 4)

    def pass_tokens(base):
        lo = send(tok.at[base + left_t, pl.ds(0, TH), :], tok.at[base + left_t, pl.ds(0, TH), :], zid(1))
        hi = send(tok.at[base + right_t, pl.ds(TH, TH), :], tok.at[base + right_t, pl.ds(TH, TH), :], zid(3))
        return [lo, hi]

    t2 = pass_tokens(yl * 4)

    jf = block(0, True)
    for cp in far_a:
        cp.wait_recv()
    yra = []
    for h in range(2):
        add(jf, h * HA, HA, [(xa.at[R, 0, 1 + h], 0), (xa.at[L, 0, 1 + h], 0)])
        yra.append(send(own(jf, h * HA, HA), ya.at[h], yfar))
    rs += yra

    ty.wait_recv()
    gy.wait_recv()
    t3 = [send(tok.at[pa_t], tok.at[pa_t], zid(k)) for k in (1, 3)]
    g3 = group(gains(pa_t), [gains(pa_t)] * 3, [zid(k) for k in (1, 2, 3)])

    near_a = a_pass(False, near_a)
    early = list(rs)

    def b_add(key, half, extra=()):
        j = block(*key)
        xx = lax.rem(x + key[0], 4)
        add(j, SA + half * HB, HB, [(yb.at[xx], half * HB), *extra])
        return j

    yrb[2].wait_recv()
    br0 = b_send(b_add((2, False), 0), 0, R, 0)
    bl0 = b_send(b_add((2, False), 1), 1, L, 0)
    yrb[1].wait_recv()
    br1 = b_send(b_add((1, False), 1), 1, R, 2)
    yrb[3].wait_recv()
    bl1 = b_send(b_add((3, False), 0), 0, L, 1)
    br0.wait_recv()
    br2 = b_send(b_add((1, False), 0, [(xb.at[R, 0], 0)]), 0, R, 1)
    bl0.wait_recv()
    bl2 = b_send(b_add((3, False), 1, [(xb.at[L, 0], 0)]), 1, L, 2)
    rs += [br0, bl0, br1, bl1, br2, bl2]

    jo = ready((0, False))

    def terms(r0, i, extra):
        v = pb[jo, rows(mine0 + r0 + i * CH, CH), :].astype(F32)
        v = v + pb[jo, rows(peer0 + r0 + i * CH, CH), :].astype(F32)
        for ref, base in extra:
            v = v + ref[rows(base + i * CH, CH), :].astype(F32)
        return v

    def squared(v):
        s = v * v
        s = s[:8] + s[8:]
        t = s[:, :128]
        for k in range(1, COLS // 128):
            t = t + s[:, k * 128:(k + 1) * 128]
        return t

    def gather_terms(r0, n, extra):
        def body(i, _):
            gf[rows(r0 + i * CH, CH), :] = terms(r0, i, extra)
            return 0

        lax.fori_loop(0, n // CH, body, 0)

    def finish(r0, n, extra, acc):
        def body(i, a):
            v = terms(r0, i, extra)
            gf[rows(r0 + i * CH, CH), :] = v
            return a + squared(v)

        return lax.fori_loop(0, n // CH, body, acc)

    def finish_last(r0, n, ref, acc):
        def body(i, a):
            r = rows(r0 + i * CH, CH)
            v = gf[r, :] + ref[rows(i * CH, CH), :].astype(F32)
            gf[r, :] = v
            return a + squared(v)

        return lax.fori_loop(0, n // CH, body, acc)

    acc = jnp.zeros((8, 128), F32)
    phase = [*early, *(cp for cps in theirs.values() for cp in cps), ty, gy, *t1]
    for cp in near_a:
        cp.wait_recv()
    for h in range(2):
        gather_terms(h * HA, HA, [(xa.at[R, 1, 1 + h], 0), (xa.at[L, 1, 1 + h], 0)])
    flush(phase)
    yrb[0].wait_recv()
    for cp in (br1, bl1, br2, bl2):
        cp.wait_recv()
    for h in range(2):
        acc = finish(SA + h * HB, HB, [(yb.at[x], h * HB), (xb.at[R, 1 + h], 0), (xb.at[L, 1 + h], 0)], acc)
    for h in range(2):
        yra[h].wait_recv()
        acc = finish_last(h * HA, HA, ya.at[h], acc)
    flush(rs)
    phase += [cp for cp in rs if id(cp) not in {id(e) for e in early}]

    slot = 0
    for stage, devs in enumerate((chips, planes)):
        nsend[stage] = acc
        n = len(devs)
        at = group(nsend.at[stage], [nrecv.at[slot + k] for k in range(n)], devs)
        if stage == 1:
            for cp in t3:
                cp.wait_recv()
            t4 = pass_tokens((1 - yl) * 4)
        group_wait(at, nrecv.at[pl.ds(slot, n)])
        for k in range(n):
            acc = acc + nrecv[slot + k]
        slot += n
    squares = jnp.sum(jnp.sum(acc, axis=0, keepdims=True), axis=1, keepdims=True)
    scale = 0.7 * math.sqrt(FF) / jnp.sqrt(squares + 1e-12)

    again += sorted((slot_of[id(cp)] for cp in phase), reverse=True)

    lw.wait()

    def perturb(i, _):
        r = rows(i * CH, CH)
        v = (wb[r, :].astype(F32) + scale * gf[r, :]).astype(BF16)
        pb[jo, rows(mine0 + i * CH, CH), :] = v
        pert[r, :] = v
        return 0

    PA, PB = GA // 2, GB // 2

    def go(j, r0, n, dev, c0=0, cn=COLS):
        ref = pb.at[j, rows(mine0 + r0, n), pl.ds(c0, cn)]
        return send(ref, ref, dev)

    d2d = {}

    def across(xk, far, r0, n, part=0, c0=0, cn=COLS):
        j = block(xk, far)
        d2d.setdefault((xk, far, part), []).append(go(j, r0, n, core, c0, cn))

    lax.fori_loop(GA // CH, BLK // CH, perturb, 0)
    ob = [go(jo, GA, GB, xdev[d]) for d in (R, L)]
    lax.fori_loop(0, GA // CH, perturb, 0)
    ya1 = go(jo, 0, GA, yfar)
    oa = [go(jo, 0, GA, xdev[d]) for d in (R, L)]
    across(0, False, 0, BLK)
    yb1 = go(jo, GA, GB, yfar)

    old = list(open_sends)

    ob[R].wait_recv()
    yl_b = go(block(3, False), GA, GB, yfar)
    across(3, False, GA, GB)
    ob[L].wait_recv()
    yr_b = go(block(1, False), GA, GB, yfar)
    across(1, False, GA, GB)
    ya1.wait_recv()
    fra = [go(block(0, True), 0, GA, xdev[d]) for d in (R, L)]
    fb = [go(block(3, False), GA, PB, xdev[R]), go(block(1, False), GA + PB, PB, xdev[L])]
    across(0, True, 0, GA)

    lt.wait()
    lg.wait()
    for cp in [*t2, *t4]:
        cp.wait_recv()
    for at in (g1, g3):
        group_wait(at, gb.at[pl.ds(0, 3 * FEAT)])
    flush([*t2, *t3, *t4])

    def norm_rows(i, _):
        r = rows(i * CH, CH)
        tot = tok[0, r, :].astype(F32)
        for k in range(1, NMP):
            tot = tot + tok[k, r, :].astype(F32)
        mean = jnp.sum(tot, axis=1, keepdims=True) * (1.0 / D)
        dev = None
        for k in range(NMP):
            e = tok[k, r, :].astype(F32) - mean
            dev = e * e if dev is None else dev + e * e
        var = jnp.sum(dev, axis=1, keepdims=True) * (1.0 / D)
        inv = 1.0 / jnp.sqrt(var + 1e-6)
        for k in range(NMP):
            e = (tok[k, r, :].astype(F32) - mean) * inv * gb[pl.ds(k * GPAD, FEAT)].astype(F32).reshape(1, FEAT)
            tok[k, r, :] = e.astype(BF16)
        return 0

    lax.fori_loop(0, TOK // CH, norm_rows, 0)

    def dots(j, n):
        cols = pl.ds(pl.multiple_of(n * NT, NT), NT)
        return jnp.dot(tok[j], pb[j, :, cols], preferred_element_type=F32)

    def multiply(xk, far, first=False, lo=0, hi=COLS):
        j = block(xk, far)
        if lo == 0:
            for cp in d2d[xk, far, 0]:
                cp.wait_recv()

        def body(n, _):
            cols = pl.ds(pl.multiple_of(n * NT, NT), NT)
            if first:
                pre[:, cols] = dots(j, n)
            else:
                pre[:, cols] = pre[:, cols] + dots(j, n)
            return 0

        lax.fori_loop(lo // NT, hi // NT, body, 0, unroll=3)

    oa[R].wait_recv()
    fa = [go(block(3, False), 0, PA, xdev[R])]
    across(3, False, 0, GA)
    oa[L].wait_recv()
    fa.append(go(block(1, False), PA, PA, xdev[L]))
    across(1, False, 0, GA)
    yb1.wait_recv()
    across(0, True, GA, GB)
    multiply(0, False, True)
    multiply(0, True)
    multiply(3, False)
    multiply(1, False)
    flush(old)
    CN = 2 * COLS // 3
    cuts = ((0, CN), (CN, COLS - CN))
    fra[R].wait_recv()
    ffa = [[go(block(3, True), 0, PA, xdev[R], *q) for q in cuts]]
    across(3, True, 0, GA)
    fra[L].wait_recv()
    ffa.append([go(block(1, True), PA, PA, xdev[L], *q) for q in cuts])
    across(1, True, 0, GA)
    y2 = []
    for k in range(2):
        fb[k].wait_recv()
        y2.append(go(block(2, False), GA + k * PB, PB, yfar))
        across(2, False, GA + k * PB, PB)
    yl_b.wait_recv()
    across(3, True, GA, GB)
    yr_b.wait_recv()
    across(1, True, GA, GB)
    multiply(3, True)
    multiply(1, True)
    for k in range(2):
        fa[k].wait_recv()
        across(2, False, k * PA, PA)
    older = [*fra, *fb, yl_b, yr_b, *fa, *d2d[3, True, 0], *d2d[1, True, 0], *d2d[2, False, 0]]
    multiply(2, False, False, 0, COLS // 2)
    for k in range(2):
        y2[k].wait_recv()
        across(2, True, GA + k * PB, PB)
    for k in range(2):
        ffa[k][0].wait_recv()
        across(2, True, k * PA, PA, 0, *cuts[0])
    multiply(2, False, False, COLS // 2, COLS)
    flush(older)
    jl = block(2, True)

    def last(n, _):
        cols = pl.ds(pl.multiple_of(n * NT, NT), NT)
        v = pre[:, cols] + dots(jl, n)
        hid[:, cols] = (v * 0.5 * (1.0 + lax.erf(v * (1.0 / math.sqrt(2.0))))).astype(BF16)
        return 0

    def finish_columns(lo, hi):
        lax.fori_loop(lo // NT, hi // NT, last, 0, unroll=2)

    for cp in d2d[2, True, 0]:
        cp.wait_recv()
    finish_columns(0, CN // 2)
    for k in range(2):
        ffa[k][1].wait_recv()
        across(2, True, k * PA, PA, 1, *cuts[1])
    finish_columns(CN // 2, CN)
    for cp in d2d[2, True, 1]:
        cp.wait_recv()
    finish_columns(CN, COLS)
    flush(open_sends)
    assert count["s"] <= NSEM and count["l"] == 11, count


def per_device(tokens, ln_gain, weights, grad_partials):
    hbm = pl.BlockSpec(memory_space=pltpu.HBM)
    return pl.pallas_call(
        kernel,
        out_shape=(
            pltpu.VMEM((TOK, COLS), BF16),
            pltpu.VMEM((BLK, COLS), BF16),
        ),
        in_specs=[hbm] * 4,
        out_specs=(pl.BlockSpec(memory_space=pltpu.VMEM),) * 2,
        scratch_shapes=[
            pltpu.VMEM((8, 2 * BLK, COLS), BF16),
            pltpu.VMEM((2, 2, 3, SA // 2, COLS), BF16),
            pltpu.VMEM((2, 3, SB // 2, COLS), BF16),
            pltpu.VMEM((2, SA // 2, COLS), BF16),
            pltpu.VMEM((4, SB, COLS), BF16),
            pltpu.VMEM((NMP, TOK, FEAT), BF16),
            pltpu.VMEM((NMP * GPAD,), BF16),
            pltpu.VMEM((BLK, COLS), F32),
            pltpu.VMEM((BLK, COLS), BF16),
            pltpu.VMEM((TOK, COLS), F32),
            pltpu.VMEM((2, 8, 128), F32),
            pltpu.VMEM((22, 8, 128), F32),
            pltpu.SemaphoreType.DMA((NSEM,)),
            pltpu.SemaphoreType.DMA((NSEM,)),
            pltpu.SemaphoreType.DMA((11,)),
        ],
        compiler_params=pltpu.CompilerParams(
            collective_id=0, has_side_effects=True, vmem_limit_bytes=63500288
        ),
    )(tokens, ln_gain, weights, grad_partials)


def solution(mesh):
    torus = Mesh(mesh.devices.reshape(4, 2, 2, 2, 4), AXES)
    placed = (P(DP, MP), P(MP), P(DP, MP), P(DP, None, MP))
    return jax.shard_map(
        per_device, mesh=torus, in_specs=placed, out_specs=(P(DP, MP), P(DP, MP)), check_vma=False
    )
```

```python
import functools
import math

import jax
import jax.numpy as jnp
from jax import lax
from jax.experimental import pallas as pl
from jax.experimental.pallas import tpu as pltpu
from jax.sharding import Mesh
from jax.sharding import PartitionSpec as P

FF = 12288
MP = ("mp_0", "mp_1")
DP = ("dp_0", "dp_1", "dp_2")
AXES = ("dp_0", "dp_1", "dp_2", "mp_0", "mp_1")
MESH = pl.DeviceIdType.MESH

BLK = 384
COLS = 1536
TOK = 768
FEAT = 768
NMP = 8
D = FEAT * NMP
SA = 288
SB = BLK - SA
GA = 224
GB = BLK - GA
CH = 16
NT = 256
NSEM = 52
GPAD = 1024
F32 = jnp.float32
BF16 = jnp.bfloat16
R, L = 0, 1


def kernel(
    tok_hbm, gain_hbm, w_hbm, grad_hbm, hid, pert,
    pb, xa, xb, ya, yb, tok, gb, gf, wb, pre, nsend, nrecv,
    ssem, rsem, lsem,
):
    x, yh, c, yl, z = [lax.axis_index(a) for a in AXES]
    y = yh * 2 + yl

    def xid(k):
        return {"dp_0": lax.rem(x + k, 4)}

    def yid(k):
        yy = lax.rem(y + k, 4)
        return {"dp_1": yy // 2, "mp_0": lax.rem(yy, 2)}

    def zid(k):
        return {"mp_1": lax.rem(z + k, 4)}

    core = {"dp_2": 1 - c}
    ypair = {"mp_0": 1 - yl}
    yfar = {"dp_1": 1 - yh}
    xdev = (xid(1), xid(3))

    count = {"s": 0, "l": 0}
    open_sends = []
    closed = set()
    again = []
    slot_of = {}

    def send(src, dst, dev, at=None):
        if at is None:
            at = again.pop() if again else count["s"]
            if at == count["s"]:
                count["s"] += 1
        i = at
        cp = pltpu.make_async_remote_copy(
            src_ref=src, dst_ref=dst, send_sem=ssem.at[i], recv_sem=rsem.at[i],
            device_id=dev, device_id_type=MESH,
        )
        cp.start()
        open_sends.append(cp)
        slot_of[id(cp)] = i
        return cp

    def group(src, dsts, devs):
        at = count["s"]
        count["s"] += 1
        for dst, dev in zip(dsts, devs):
            closed.add(id(send(src, dst, dev, at)))
        return at

    def group_wait(at, ref):
        cp = pltpu.make_async_remote_copy(
            src_ref=ref, dst_ref=ref, send_sem=ssem.at[at], recv_sem=rsem.at[at],
            device_id=core, device_id_type=MESH,
        )
        cp.wait_recv()
        cp.wait_send()

    def flush(cps):
        for cp in cps:
            if id(cp) not in closed:
                closed.add(id(cp))
                cp.wait_send()

    def local(src, dst):
        i = count["l"]
        count["l"] += 1
        cp = pltpu.make_async_copy(src, dst, lsem.at[i])
        cp.start()
        return cp

    def rows(start, n):
        return pl.ds(pl.multiple_of(start, 16), n)

    mine0 = c * BLK
    peer0 = (1 - c) * BLK
    peer_dst = c * BLK

    def block(xk, far):
        return lax.rem(x + xk, 4) * 2 + ((1 - yh) if far else yh)

    def own(j, r0, n):
        return pb.at[j, rows(mine0 + r0, n), :]

    barrier = pltpu.get_barrier_semaphore()
    chips = [core, *(xid(k) for k in (1, 2, 3)), *({**xid(k), **core} for k in (1, 2, 3))]
    planes = [{**yid(i), **zid(k)} for i in range(4) for k in range(4) if i or k]
    peers = chips + planes
    for p in peers:
        pl.semaphore_signal(barrier, inc=1, device_id=p, device_id_type=MESH)
    order = [(2, True), (1, True), (3, True), (0, True), (2, False), (1, False), (3, False), (0, False)]
    mine = {}
    for key in order:
        j = block(*key)
        mine[key] = local(grad_hbm.at[0, rows(2 * j * BLK + mine0, BLK), :], own(j, 0, BLK))
    me_t, pa_t = yl * 4 + z, (1 - yl) * 4 + z
    def gains(k):
        return gb.at[pl.ds(pl.multiple_of(k * GPAD, GPAD), FEAT)]

    lt = local(tok_hbm, tok.at[me_t])
    lg = local(gain_hbm, gains(me_t))
    lw = local(w_hbm, wb)
    pl.semaphore_wait(barrier, len(peers))

    theirs = {}
    HA, HB = SA // 2, SB // 2
    for key in order:
        j = block(*key)
        cuts = (0, HA, SA, BLK) if key == order[0] else (0, BLK)
        theirs[key] = [
            send(grad_hbm.at[0, rows(2 * j * BLK + peer0 + lo, hi - lo), :], pb.at[j, rows(peer_dst + lo, hi - lo), :], core)
            for lo, hi in zip(cuts, cuts[1:])
        ]
    ty = send(tok_hbm, tok.at[me_t], ypair)
    t1 = [send(tok_hbm, tok.at[me_t], zid(k)) for k in (1, 3)]
    gy = send(gain_hbm, gains(me_t), ypair)
    g1 = group(gain_hbm, [gains(me_t)] * 3, [zid(k) for k in (1, 2, 3)])

    def add(j, r0, n, extra=()):
        def body(i, _):
            r = rows(mine0 + r0 + i * CH, CH)
            v = pb[j, r, :].astype(F32) + pb[j, rows(peer0 + r0 + i * CH, CH), :].astype(F32)
            for ref, base in extra:
                v = v + ref[rows(base + i * CH, CH), :].astype(F32)
            pb[j, r, :] = v.astype(BF16)
            return 0

        lax.fori_loop(0, n // CH, body, 0, unroll=3)

    def ready(key, first=0):
        if not first:
            mine[key].wait()
        theirs[key][first].wait_recv()
        return block(*key)

    def a_send(j, near, half, d, slot):
        return send(own(j, half * HA, HA), xa.at[d, near, slot], xdev[d])

    def b_send(j, half, d, slot):
        return send(own(j, SA + half * HB, HB), xb.at[d, slot], xdev[d])

    rs = []

    def y_send(key):
        j = block(*key)
        xx = lax.rem(x + key[0], 4)
        add(j, SA, SB)
        cp = send(own(j, SA, SB), yb.at[xx], yfar)
        rs.append(cp)
        return cp

    def a_open(far):
        near = 0 if far else 1
        j = ready((2, far))
        add(j, 0, HA)
        r0 = a_send(j, near, 0, R, 0)
        if far:
            ready((2, far), 1)
        add(j, HA, HA)
        l0 = a_send(j, near, 1, L, 0)
        j = ready((1, far))
        add(j, HA, HA)
        r1 = a_send(j, near, 1, R, 2)
        j = ready((3, far))
        add(j, 0, HA)
        l1 = a_send(j, near, 0, L, 1)
        rs.extend((r0, l0, r1, l1))
        return r0, l0, r1, l1

    def a_pass(far, opened):
        near = 0 if far else 1
        r0, l0, r1, l1 = opened
        jr, jl = block(1, far), block(3, far)
        r0.wait_recv()
        add(jr, 0, HA, [(xa.at[R, near, 0], 0)])
        r2 = a_send(jr, near, 0, R, 1)
        l0.wait_recv()
        add(jl, HA, HA, [(xa.at[L, near, 0], 0)])
        l2 = a_send(jl, near, 1, L, 2)
        rs.extend((r2, l2))
        return r1, r2, l1, l2

    far_a = a_open(True)
    yrb = {}
    ready((2, True), 2)
    for xk in (2, 1, 3):
        yrb[xk] = y_send((xk, True))
    ready((0, True))
    yrb[0] = y_send((0, True))
    far_a = a_pass(True, far_a)
    near_a = a_open(False)

    for cp in t1:
        cp.wait_recv()
    TH = TOK // 2
    left_t, right_t = lax.rem(z + 3, 4), lax.rem(z + 1, 4)

    def pass_tokens(base):
        lo = send(tok.at[base + left_t, pl.ds(0, TH), :], tok.at[base + left_t, pl.ds(0, TH), :], zid(1))
        hi = send(tok.at[base + right_t, pl.ds(TH, TH), :], tok.at[base + right_t, pl.ds(TH, TH), :], zid(3))
        return [lo, hi]

    t2 = pass_tokens(yl * 4)

    jf = block(0, True)
    for cp in far_a:
        cp.wait_recv()
    yra = []
    for h in range(2):
        add(jf, h * HA, HA, [(xa.at[R, 0, 1 + h], 0), (xa.at[L, 0, 1 + h], 0)])
        yra.append(send(own(jf, h * HA, HA), ya.at[h], yfar))
    rs += yra

    ty.wait_recv()
    gy.wait_recv()
    t3 = [send(tok.at[pa_t], tok.at[pa_t], zid(k)) for k in (1, 3)]
    g3 = group(gains(pa_t), [gains(pa_t)] * 3, [zid(k) for k in (1, 2, 3)])

    near_a = a_pass(False, near_a)
    early = list(rs)

    def b_add(key, half, extra=()):
        j = block(*key)
        xx = lax.rem(x + key[0], 4)
        add(j, SA + half * HB, HB, [(yb.at[xx], half * HB), *extra])
        return j

    yrb[2].wait_recv()
    br0 = b_send(b_add((2, False), 0), 0, R, 0)
    bl0 = b_send(b_add((2, False), 1), 1, L, 0)
    yrb[1].wait_recv()
    br1 = b_send(b_add((1, False), 1), 1, R, 2)
    yrb[3].wait_recv()
    bl1 = b_send(b_add((3, False), 0), 0, L, 1)
    br0.wait_recv()
    br2 = b_send(b_add((1, False), 0, [(xb.at[R, 0], 0)]), 0, R, 1)
    bl0.wait_recv()
    bl2 = b_send(b_add((3, False), 1, [(xb.at[L, 0], 0)]), 1, L, 2)
    rs += [br0, bl0, br1, bl1, br2, bl2]

    jo = ready((0, False))

    def terms(r0, i, extra):
        v = pb[jo, rows(mine0 + r0 + i * CH, CH), :].astype(F32)
        v = v + pb[jo, rows(peer0 + r0 + i * CH, CH), :].astype(F32)
        for ref, base in extra:
            v = v + ref[rows(base + i * CH, CH), :].astype(F32)
        return v

    def squared(v):
        s = v * v
        s = s[:8] + s[8:]
        t = s[:, :128]
        for k in range(1, COLS // 128):
            t = t + s[:, k * 128:(k + 1) * 128]
        return t

    def gather_terms(r0, n, extra):
        def body(i, _):
            gf[rows(r0 + i * CH, CH), :] = terms(r0, i, extra)
            return 0

        lax.fori_loop(0, n // CH, body, 0)

    def finish(r0, n, extra, acc):
        def body(i, a):
            v = terms(r0, i, extra)
            gf[rows(r0 + i * CH, CH), :] = v
            return a + squared(v)

        return lax.fori_loop(0, n // CH, body, acc, unroll=3)

    def finish_last(r0, n, ref, acc):
        def body(i, a):
            r = rows(r0 + i * CH, CH)
            v = gf[r, :] + ref[rows(i * CH, CH), :].astype(F32)
            gf[r, :] = v
            return a + squared(v)

        return lax.fori_loop(0, n // CH, body, acc, unroll=3)

    acc = jnp.zeros((8, 128), F32)
    phase = [*early, *(cp for cps in theirs.values() for cp in cps), ty, gy, *t1]
    for cp in near_a:
        cp.wait_recv()
    for h in range(2):
        gather_terms(h * HA, HA, [(xa.at[R, 1, 1 + h], 0), (xa.at[L, 1, 1 + h], 0)])
    flush(phase)
    yrb[0].wait_recv()
    for cp in (br1, bl1, br2, bl2):
        cp.wait_recv()
    for h in range(2):
        acc = finish(SA + h * HB, HB, [(yb.at[x], h * HB), (xb.at[R, 1 + h], 0), (xb.at[L, 1 + h], 0)], acc)
    for h in range(2):
        yra[h].wait_recv()
        acc = finish_last(h * HA, HA, ya.at[h], acc)
    flush(rs)
    phase += [cp for cp in rs if id(cp) not in {id(e) for e in early}]

    slot = 0
    for stage, devs in enumerate((chips, planes)):
        nsend[stage] = acc
        n = len(devs)
        at = group(nsend.at[stage], [nrecv.at[slot + k] for k in range(n)], devs)
        if stage == 1:
            for cp in t3:
                cp.wait_recv()
            t4 = pass_tokens((1 - yl) * 4)
        group_wait(at, nrecv.at[pl.ds(slot, n)])
        for k in range(n):
            acc = acc + nrecv[slot + k]
        slot += n
    squares = jnp.sum(jnp.sum(acc, axis=0, keepdims=True), axis=1, keepdims=True)
    scale = 0.7 * math.sqrt(FF) / jnp.sqrt(squares + 1e-12)

    again += sorted((slot_of[id(cp)] for cp in phase), reverse=True)

    lw.wait()

    def perturb(i, _):
        r = rows(i * CH, CH)
        v = (wb[r, :].astype(F32) + scale * gf[r, :]).astype(BF16)
        pb[jo, rows(mine0 + i * CH, CH), :] = v
        pert[r, :] = v
        return 0

    PA, PB = GA // 2, GB // 2

    def go(j, r0, n, dev, c0=0, cn=COLS):
        ref = pb.at[j, rows(mine0 + r0, n), pl.ds(c0, cn)]
        return send(ref, ref, dev)

    d2d = {}

    def across(xk, far, r0, n, part=0, c0=0, cn=COLS):
        j = block(xk, far)
        d2d.setdefault((xk, far, part), []).append(go(j, r0, n, core, c0, cn))

    lax.fori_loop(GA // CH, BLK // CH, perturb, 0, unroll=2)
    ob = [go(jo, GA, GB, xdev[d]) for d in (R, L)]
    lax.fori_loop(0, GA // CH, perturb, 0, unroll=2)
    ya1 = go(jo, 0, GA, yfar)
    oa = [go(jo, 0, GA, xdev[d]) for d in (R, L)]
    across(0, False, 0, BLK)
    yb1 = go(jo, GA, GB, yfar)

    old = list(open_sends)

    ob[R].wait_recv()
    yl_b = go(block(3, False), GA, GB, yfar)
    across(3, False, GA, GB)
    ob[L].wait_recv()
    yr_b = go(block(1, False), GA, GB, yfar)
    across(1, False, GA, GB)
    ya1.wait_recv()
    fra = [go(block(0, True), 0, GA, xdev[d]) for d in (R, L)]
    fb = [go(block(3, False), GA, PB, xdev[R]), go(block(1, False), GA + PB, PB, xdev[L])]
    across(0, True, 0, GA)

    lt.wait()
    lg.wait()
    for cp in [*t2, *t4]:
        cp.wait_recv()
    for at in (g1, g3):
        group_wait(at, gb.at[pl.ds(0, 3 * FEAT)])
    flush([*t2, *t3, *t4])

    def norm_rows(i, _):
        r = rows(i * CH, CH)
        tot = tok[0, r, :].astype(F32)
        for k in range(1, NMP):
            tot = tot + tok[k, r, :].astype(F32)
        mean = jnp.sum(tot, axis=1, keepdims=True) * (1.0 / D)
        dev = None
        for k in range(NMP):
            e = tok[k, r, :].astype(F32) - mean
            dev = e * e if dev is None else dev + e * e
        var = jnp.sum(dev, axis=1, keepdims=True) * (1.0 / D)
        inv = 1.0 / jnp.sqrt(var + 1e-6)
        for k in range(NMP):
            e = (tok[k, r, :].astype(F32) - mean) * inv * gb[pl.ds(k * GPAD, FEAT)].astype(F32).reshape(1, FEAT)
            tok[k, r, :] = e.astype(BF16)
        return 0

    lax.fori_loop(0, TOK // CH, norm_rows, 0)

    def dots(j, n):
        cols = pl.ds(pl.multiple_of(n * NT, NT), NT)
        return jnp.dot(tok[j], pb[j, :, cols], preferred_element_type=F32)

    def multiply(xk, far, first=False, lo=0, hi=COLS):
        j = block(xk, far)
        if lo == 0:
            for cp in d2d[xk, far, 0]:
                cp.wait_recv()

        def body(n, _):
            cols = pl.ds(pl.multiple_of(n * NT, NT), NT)
            if first:
                pre[:, cols] = dots(j, n)
            else:
                pre[:, cols] = pre[:, cols] + dots(j, n)
            return 0

        lax.fori_loop(lo // NT, hi // NT, body, 0, unroll=3)

    oa[R].wait_recv()
    fa = [go(block(3, False), 0, PA, xdev[R])]
    across(3, False, 0, GA)
    oa[L].wait_recv()
    fa.append(go(block(1, False), PA, PA, xdev[L]))
    across(1, False, 0, GA)
    yb1.wait_recv()
    across(0, True, GA, GB)
    multiply(0, False, True)
    multiply(0, True)
    multiply(3, False)
    multiply(1, False)
    flush(old)
    CN = 2 * COLS // 3
    cuts = ((0, CN), (CN, COLS - CN))
    fra[R].wait_recv()
    ffa = [[go(block(3, True), 0, PA, xdev[R], *q) for q in cuts]]
    across(3, True, 0, GA)
    fra[L].wait_recv()
    ffa.append([go(block(1, True), PA, PA, xdev[L], *q) for q in cuts])
    across(1, True, 0, GA)
    y2 = []
    for k in range(2):
        fb[k].wait_recv()
        y2.append(go(block(2, False), GA + k * PB, PB, yfar))
        across(2, False, GA + k * PB, PB)
    yl_b.wait_recv()
    across(3, True, GA, GB)
    yr_b.wait_recv()
    across(1, True, GA, GB)
    multiply(3, True)
    multiply(1, True)
    for k in range(2):
        fa[k].wait_recv()
        across(2, False, k * PA, PA)
    older = [*fra, *fb, yl_b, yr_b, *fa, *d2d[3, True, 0], *d2d[1, True, 0], *d2d[2, False, 0]]
    multiply(2, False, False, 0, COLS // 2)
    for k in range(2):
        y2[k].wait_recv()
        across(2, True, GA + k * PB, PB)
    for k in range(2):
        ffa[k][0].wait_recv()
        across(2, True, k * PA, PA, 0, *cuts[0])
    multiply(2, False, False, COLS // 2, COLS)
    flush(older)
    jl = block(2, True)

    def last(n, _):
        cols = pl.ds(pl.multiple_of(n * NT, NT), NT)
        v = pre[:, cols] + dots(jl, n)
        hid[:, cols] = (v * 0.5 * (1.0 + lax.erf(v * (1.0 / math.sqrt(2.0))))).astype(BF16)
        return 0

    def finish_columns(lo, hi):
        lax.fori_loop(lo // NT, hi // NT, last, 0, unroll=2)

    for cp in d2d[2, True, 0]:
        cp.wait_recv()
    finish_columns(0, CN // 2)
    for k in range(2):
        ffa[k][1].wait_recv()
        across(2, True, k * PA, PA, 1, *cuts[1])
    finish_columns(CN // 2, CN)
    for cp in d2d[2, True, 1]:
        cp.wait_recv()
    finish_columns(CN, COLS)
    flush(open_sends)
    assert count["s"] <= NSEM and count["l"] == 11, count


def per_device(tokens, ln_gain, weights, grad_partials):
    hbm = pl.BlockSpec(memory_space=pltpu.HBM)
    return pl.pallas_call(
        kernel,
        out_shape=(
            pltpu.VMEM((TOK, COLS), BF16),
            pltpu.VMEM((BLK, COLS), BF16),
        ),
        in_specs=[hbm] * 4,
        out_specs=(pl.BlockSpec(memory_space=pltpu.VMEM),) * 2,
        scratch_shapes=[
            pltpu.VMEM((8, 2 * BLK, COLS), BF16),
            pltpu.VMEM((2, 2, 3, SA // 2, COLS), BF16),
            pltpu.VMEM((2, 3, SB // 2, COLS), BF16),
            pltpu.VMEM((2, SA // 2, COLS), BF16),
            pltpu.VMEM((4, SB, COLS), BF16),
            pltpu.VMEM((NMP, TOK, FEAT), BF16),
            pltpu.VMEM((NMP * GPAD,), BF16),
            pltpu.VMEM((BLK, COLS), F32),
            pltpu.VMEM((BLK, COLS), BF16),
            pltpu.VMEM((TOK, COLS), F32),
            pltpu.VMEM((2, 8, 128), F32),
            pltpu.VMEM((22, 8, 128), F32),
            pltpu.SemaphoreType.DMA((NSEM,)),
            pltpu.SemaphoreType.DMA((NSEM,)),
            pltpu.SemaphoreType.DMA((11,)),
        ],
        compiler_params=pltpu.CompilerParams(
            collective_id=0, has_side_effects=True, vmem_limit_bytes=63500288
        ),
    )(tokens, ln_gain, weights, grad_partials)


def solution(mesh):
    torus = Mesh(mesh.devices.reshape(4, 2, 2, 2, 4), AXES)
    placed = (P(DP, MP), P(MP), P(DP, MP), P(DP, None, MP))
    return jax.shard_map(
        per_device, mesh=torus, in_specs=placed, out_specs=(P(DP, MP), P(DP, MP)), check_vma=False
    )
```
